32 devices in a mesh: role: 2 (over x), grp: 8 (over z, y), tp: 2 (over core).
Axes of the slice: x: 2, y: 2, z: 4, core: 2. Of those that a mesh axis runs over, the one named last changes fastest.
Arguments:
- q_new: bfloat16 [256, 4096], P('grp', ('role', 'tp')), may hold values from -9 to 9
- k_new: bfloat16 [256, 512], P('grp', ('role', 'tp')), may hold values from -6 to 6
- v_new: bfloat16 [256, 512], P('grp', ('role', 'tp')), may hold values from -6 to 6
- k_cache: bfloat16 [256, 128, 512], P('grp', None, ('role', 'tp')), may hold values from -9 to 9
- v_cache: bfloat16 [256, 128, 512], P('grp', None, ('role', 'tp')), may hold values from -6 to 6
- cache_len: int32 [256], P('grp'), may hold values from 1 to 127
- cycle_start: int32 [256], P('grp'), may hold values from 0 to 127
- residual: bfloat16 [256, 2880], P('grp', ('role', 'tp')), may hold values from -6 to 6
- out_proj: bfloat16 [4096, 2880], P(('role', 'tp')), may hold values from -0.09375 to 0.09375
- norm_gain: float32 [2880], replicated, may hold values from 0.25 to 1.75
- router: bfloat16 [2880, 8], P(('role', 'tp')), may hold values from -0.21875 to 0.21875
- route_ids: int32 [256, 4], P('grp'), may hold values from 0 to 7, all different within a row; in each aligned block of 32 rows (0 to 31, 32 to 63, ...) at most 18 rows name the same one
- w_gate: bfloat16 [8, 2880, 1440], P('grp', None, ('role', 'tp')), may hold values from -0.109375 to 0.109375
- w_up: bfloat16 [8, 2880, 1440], P('grp', None, ('role', 'tp')), may hold values from -0.109375 to 0.109375
- w_down: bfloat16 [8, 1440, 2880], P('grp', ('role', 'tp')), may hold values from -0.15625 to 0.15625
Outputs:
- attended: bfloat16 [256, 2880], P('grp', ('role', 'tp'))
- expert_mix: bfloat16 [256, 2880], P('grp', ('role', 'tp'))
The draws below stay inside these ranges and needn't reach their ends.
Inputs may be any that keep to these rules, and one draw needn't show every extreme that they name: `route_ids`: the 4 experts of a token differ. Among the tokens of one grp index (aligned blocks of 32 tokens) no expert is named more than 18 times, a bound that some block reaches.
All inputs are finite; a program needn't handle non-finite values.
Results may differ from the reference program's by a relative error of at most 0.017.
Values may be sent and summed in bfloat16 or wider, within the bound.
No kernel may reach another device: no remote copies, remote signals or barrier semaphores. Data moves between devices by JAX's collectives and lax.ppermute only.
A program may use at most 64 MiB of HBM per device.

```python
import math
import jax
import jax.numpy as jnp
import numpy as np
from jax import lax

D = 2880
FF = 1440
HEADS = 64
KV_HEADS = 8
HD = 64
WINDOW = 128
TOPK = 4
TOK_DEV = 32
TOKENS = 256
EXPERTS = 8
CAP = 18
N_ROLE = 2
N_GRP = 8
N_TP = 2


def draw_q_new(key, part):
    return jnp.clip(jax.random.normal(jax.random.fold_in(key, 11), (TOKENS, HEADS * HD), jnp.float32), -6.0, 6.0).astype(jnp.bfloat16)


def draw_k_cache(key, part):
    return jnp.clip(jax.random.normal(jax.random.fold_in(key, 13), (TOKENS, WINDOW, KV_HEADS * HD), jnp.float32), -6.0, 6.0).astype(jnp.bfloat16)


def place_ends(values, key, least, high):
    shape = values.shape
    spot = [jax.random.randint(jax.random.fold_in(key, axis), (), 0, shape[axis]) for axis in range(len(shape))]
    values = values.at[tuple(spot)].set(least)
    longest = shape.index(max(shape))
    spot[longest] = (spot[longest] + 1) % shape[longest]
    return values.at[tuple(spot)].set(high)


def levels(stream_key, shape, split, low, top_value):
    level = 1.0
    for position, blocks in split:
        steps = jax.random.uniform(jax.random.fold_in(jax.random.fold_in(stream_key, 6), position), (blocks,), jnp.float32, low / len(split), top_value / len(split))
        level = level * jnp.repeat(jnp.exp(steps), shape[position] // blocks).reshape((-1,) + (1,) * (len(shape) - 1 - position))
    return level


def deal_out(rng, own, number, rows, count, top, reach, slope):
    order = jax.random.permutation(rng, count)
    packed, ordinary = portions_of(count, rows * top, reach, slope, True), portions_of(count, rows * top, reach, slope, False)
    places = jnp.arange(count)

    def named(tallies, rotation):
        used = int((tallies > 0).sum())
        fixed = max(1, used // 4)
        passed = fixed + (places - fixed + rotation * (used - fixed)) % max(1, count - fixed)
        return jnp.zeros((count,), jnp.int32).at[order[jnp.where(places < fixed, places, passed)]].set(jnp.asarray(tallies, jnp.int32))

    tallies = jnp.where(number % 4 == 0, named(packed, number // 4), named(ordinary, number - number // 4 - 1))
    mixed = jax.random.permutation(jax.random.fold_in(own, 3), count)
    source_of, receiver = mixed[0:count // 2 * 2:2], mixed[1:count // 2 * 2:2]
    slack = jnp.minimum(tallies[source_of] - 1, reach - tallies[receiver]) // 2
    slack = jnp.where((source_of == order[0]) | (receiver == order[0]) | (tallies[receiver] == 0), 0, jnp.maximum(slack, 0))
    passed = jax.random.randint(jax.random.fold_in(own, 4), (count // 2,), 0, 1 << 20) % (slack + 1)
    tallies = tallies.at[source_of].add(-passed).at[receiver].add(passed)
    items = jnp.searchsorted(jnp.cumsum(tallies), jnp.arange(rows * top), side="right").astype(jnp.int32)
    table = items.reshape(top, rows).T
    table = table[jax.random.permutation(jax.random.fold_in(own, 1), rows)]
    rotation = jax.random.randint(jax.random.fold_in(own, 2), (rows, 1), 0, top)
    return jnp.take_along_axis(table, (jnp.arange(top)[None, :] + rotation) % top, axis=1)


def portions_of(count, total, limit, lean, full):
    weights = [(1 << 20) // math.isqrt(rank ** lean) + 1 for rank in range(1, count + 1)]
    largest = limit if full else min(limit, max(-(-total // count), total * weights[0] // sum(weights)))
    least = 1 if total - largest >= count - 1 else 0
    given, rest = [largest] + [least] * (count - 1), total - largest - least * (count - 1)
    while rest > 0:
        free = [i for i in range(1, count) if given[i] < largest] or [i for i in range(1, count) if given[i] < limit]
        whole, budget = sum([weights[i] for i in free]), rest
        for i in free:
            more = min(limit - given[i], max(1, budget * weights[i] // whole), rest)
            given[i] = given[i] + more
            rest = rest - more
    return np.array(given)


def normal_values(stream_key, shape, width, bound, shards=(), kind=jnp.bfloat16):
    entries = width * jax.random.normal(stream_key, shape, jnp.float32)
    if shards:
        entries = entries * levels(stream_key, shape, shards, -0.22, 0.18)
    return jnp.clip(entries, -bound, bound).astype(kind)


def setup_inputs(seed: int = 0) -> dict:
    splits = jax.random.split(jax.random.key(seed), 16)
    q_new = draw_q_new(jax.random.fold_in(splits[15], 71), 0)
    k_new = normal_values(splits[1], (TOKENS, KV_HEADS * HD), 1.0, 6.0, ((0, 8), (1, 4)))
    v_new = normal_values(splits[2], (TOKENS, KV_HEADS * HD), 1.0, 6.0, ((0, 8), (1, 4)))
    k_cache = draw_k_cache(jax.random.fold_in(splits[15], 71), 0)
    v_cache = normal_values(splits[4], (TOKENS, WINDOW, KV_HEADS * HD), 1.0, 6.0, ((0, 8), (2, 4)))
    cache_len = place_ends(jax.random.randint(splits[5], (TOKENS,), 1, WINDOW), jax.random.fold_in(splits[5], 1), 1, WINDOW - 1).astype(jnp.int32)
    cycle_start = place_ends(jax.random.randint(splits[6], (TOKENS,), 0, WINDOW), jax.random.fold_in(splits[6], 1), 0, WINDOW - 1).astype(jnp.int32)
    residual = normal_values(splits[7], (TOKENS, D), 1.0, 6.0, ((0, 8), (1, 4)))
    out_proj = normal_values(splits[8], (HEADS * HD, D), (HEADS * HD) ** -0.5, 0.09375, ((0, 4),))
    norm_gain = jnp.clip(1.0 + 0.15 * jax.random.normal(splits[9], (D,), jnp.float32), 0.25, 1.75)
    router = normal_values(splits[10], (D, EXPERTS), (D // 4) ** -0.5, 0.21875, ((0, 4),))
    route_ids_keys = jax.random.split(jax.random.fold_in(splits[11], 1), TOKENS // TOK_DEV)
    route_ids_turns = jax.random.permutation(jax.random.fold_in(splits[11], 3), TOKENS // TOK_DEV)
    route_ids = jax.vmap(lambda own, number: deal_out(jax.random.fold_in(splits[11], 2), own, number, TOK_DEV, EXPERTS, TOPK, CAP, 2))(route_ids_keys, route_ids_turns).reshape((TOKENS, TOPK))
    w_gate = normal_values(splits[12], (EXPERTS, D, FF), D ** -0.5, 0.109375, ((0, 8), (2, 4)))
    w_up = normal_values(splits[13], (EXPERTS, D, FF), D ** -0.5, 0.109375, ((0, 8), (2, 4)))
    w_down = normal_values(splits[14], (EXPERTS, FF, D), FF ** -0.5, 0.15625, ((0, 8), (1, 4)))
    return dict(q_new=q_new, k_new=k_new, v_new=v_new, k_cache=k_cache, v_cache=v_cache, cache_len=cache_len, cycle_start=cycle_start, residual=residual, out_proj=out_proj, norm_gain=norm_gain, router=router, route_ids=route_ids, w_gate=w_gate, w_up=w_up, w_down=w_down)


epsilon = 1e-05

def attend(q_new, k_new, v_new, k_cache, v_cache, cache_len, cycle_start):
    tokens = q_new.shape[0]
    window = k_cache.shape[1]
    kv_local = k_new.shape[1] // HD
    grouped = HEADS // KV_HEADS
    queries = q_new.astype(jnp.float32).reshape(tokens, kv_local, grouped, HD)
    cached_keys = k_cache.astype(jnp.float32).reshape(tokens, window, kv_local, HD)
    cached_values = v_cache.astype(jnp.float32).reshape(tokens, window, kv_local, HD)
    own_key = k_new.astype(jnp.float32).reshape(tokens, kv_local, HD)
    own_value = v_new.astype(jnp.float32).reshape(tokens, kv_local, HD)
    factor = HD ** (-0.5)
    scores = jnp.einsum('tkgd,tskd->tkgs', queries, cached_keys) * factor
    own_score = jnp.einsum('tkgd,tkd->tkg', queries, own_key) * factor
    positions = jnp.arange(window, dtype=jnp.int32)
    usable = (positions[None, :] - cycle_start[:, None]) % window < cache_len[:, None]
    usable = usable[:, None, None, :]
    masked = jnp.where(usable, scores, -1e+30)
    highest = jnp.maximum(lax.optimization_barrier(jnp.max(masked, axis=3)), own_score)
    lifted = jnp.where(usable, jnp.exp(masked - highest[..., None]), 0.0)
    own_lift = jnp.exp(own_score - highest)
    denominator = lax.optimization_barrier(jnp.sum(lifted, axis=3)) + own_lift
    weights = lax.optimization_barrier((lifted / denominator[..., None]).astype(jnp.bfloat16)).astype(jnp.float32)
    own_weight = lax.optimization_barrier((own_lift / denominator).astype(jnp.bfloat16)).astype(jnp.float32)
    combined = jnp.einsum('tkgs,tskd->tkgd', weights, cached_values)
    combined = combined + own_weight[..., None] * own_value[:, :, None, :]
    return combined.reshape(tokens, -1).astype(jnp.bfloat16)

def block_ranks(route_ids):
    named = route_ids[:, :, None] == jnp.arange(EXPERTS, dtype=jnp.int32)
    counts = lax.optimization_barrier(jnp.sum(named.astype(jnp.int32), axis=1))
    blocked = counts.reshape(-1, TOK_DEV, EXPERTS)
    earlier = (jnp.cumsum(blocked, axis=1) - blocked).reshape(-1, EXPERTS)
    return lax.optimization_barrier(jnp.sum(jnp.where(named, earlier[:, None, :], 0), axis=2)).astype(jnp.int32)

def reference(q_new, k_new, v_new, k_cache, v_cache, cache_len, cycle_start, residual, out_proj, norm_gain, router, route_ids, w_gate, w_up, w_down):
    heads_out = attend(q_new, k_new, v_new, k_cache, v_cache, cache_len, cycle_start)
    stream = residual.astype(jnp.float32) + jnp.dot(heads_out, out_proj, preferred_element_type=jnp.float32)
    scale = lax.rsqrt(lax.optimization_barrier(jnp.mean(stream * stream, axis=1, keepdims=True)) + epsilon)
    normed = (stream * scale * norm_gain).astype(jnp.bfloat16)
    logits = jnp.dot(normed, router, preferred_element_type=jnp.float32)
    chosen = jnp.take_along_axis(logits, route_ids, axis=1)
    lifted = jnp.exp(chosen)
    route_weight = lifted / lax.optimization_barrier(jnp.sum(lifted, axis=1, keepdims=True))
    ranks = block_ranks(route_ids)
    shares = N_ROLE * N_TP
    share_width = FF // shares
    grouped_ids = route_ids.reshape(N_GRP, TOK_DEV, TOPK)
    grouped_ranks = ranks.reshape(N_GRP, TOK_DEV, TOPK)
    blocks = normed.astype(jnp.float32).reshape(N_GRP, TOK_DEV, D)
    capacity_range = jnp.arange(CAP, dtype=jnp.int32)

    def serve_expert(expert):
        picked = (grouped_ids == expert)[:, :, :, None] & (grouped_ranks[:, :, :, None] == capacity_range)
        select = lax.optimization_barrier(jnp.sum(picked.astype(jnp.float32), axis=2))
        inputs = jnp.einsum('gtc,gtd->gcd', select, blocks).reshape(N_GRP * CAP, D).astype(jnp.bfloat16)
        gate_lin = jnp.dot(inputs, w_gate[expert], preferred_element_type=jnp.float32)
        up_lin = jnp.dot(inputs, w_up[expert], preferred_element_type=jnp.float32)
        activated = (gate_lin * jax.nn.sigmoid(1.702 * gate_lin) * (up_lin + 1.0)).astype(jnp.bfloat16)
        pieces = jnp.einsum('nsf,sfd->snd', activated.astype(jnp.float32).reshape(-1, shares, share_width), w_down[expert].astype(jnp.float32).reshape(shares, share_width, D))
        rounded = lax.optimization_barrier(pieces.astype(jnp.bfloat16)).astype(jnp.float32)
        return lax.optimization_barrier(jnp.sum(rounded, axis=0))
    outputs = lax.map(serve_expert, jnp.arange(EXPERTS, dtype=jnp.int32))
    source = (jnp.arange(TOKENS, dtype=jnp.int32) // TOK_DEV)[:, None]
    gathered = outputs[route_ids, source * CAP + ranks]
    expert_mix = lax.optimization_barrier(jnp.sum(route_weight[:, :, None] * gathered, axis=1))
    return (stream.astype(jnp.bfloat16), expert_mix.astype(jnp.bfloat16))
```

```python
import math

import jax
import jax.numpy as jnp
import numpy as np
from jax import lax
from jax.sharding import PartitionSpec as P

HEADS = 64
KV_HEADS = 8
HD = 64


epsilon = 1e-05


def attend(q_new, k_new, v_new, k_cache, v_cache, cache_len, cycle_start):
    tokens = q_new.shape[0]
    window = k_cache.shape[1]
    kv_local = k_new.shape[1] // HD
    grouped = HEADS // KV_HEADS
    queries = q_new.reshape(tokens, kv_local, grouped, HD)
    cached_keys = k_cache.reshape(tokens, window, kv_local, HD)
    cached_values = v_cache.reshape(tokens, window, kv_local, HD)
    own_key = k_new.reshape(tokens, kv_local, HD)
    own_value = v_new.reshape(tokens, kv_local, HD)
    factor = HD ** (-0.5)
    scores = (
        jnp.einsum("tkgd,tskd->tkgs", queries, cached_keys, preferred_element_type=jnp.float32)
        * factor
    )
    own_score = (
        jnp.einsum("tkgd,tkd->tkg", queries, own_key, preferred_element_type=jnp.float32) * factor
    )
    positions = jnp.arange(window, dtype=jnp.int32)
    usable = (positions[None, :] - cycle_start[:, None]) % window < cache_len[:, None]
    usable = usable[:, None, None, :]
    masked = jnp.where(usable, scores, -1e30)
    highest = jnp.maximum(jnp.max(masked, axis=3), own_score)
    lifted = jnp.where(usable, jnp.exp(masked - highest[..., None]), 0.0)
    own_lift = jnp.exp(own_score - highest)
    denominator = jnp.sum(lifted, axis=3) + own_lift
    weights = (lifted / denominator[..., None]).astype(jnp.bfloat16)
    own_weight = (own_lift / denominator).astype(jnp.bfloat16)
    combined = jnp.einsum(
        "tkgs,tskd->tkgd", weights, cached_values, preferred_element_type=jnp.float32
    )
    combined = (
        combined
        + own_weight.astype(jnp.float32)[..., None] * own_value.astype(jnp.float32)[:, :, None, :]
    )
    return combined.reshape(tokens, -1).astype(jnp.bfloat16)


def split3(x):
    high = lax.reduce_precision(x, 8, 7)
    rest = x - high
    middle = lax.reduce_precision(rest, 8, 7)
    low = rest - middle
    return [part.astype(jnp.bfloat16) for part in (high, middle, low)]


def swap_table(mesh, grp_of, role_flip, tp_flip):
    names = mesh.axis_names
    sizes = [mesh.shape[n] for n in names]
    pairs = []
    for flat in range(math.prod(sizes)):
        at = dict(zip(names, [int(v) for v in np.unravel_index(flat, sizes)]))
        to = dict(
            role=at["role"] ^ role_flip, tp=at["tp"] ^ tp_flip, grp=grp_of(at["grp"])
        )
        pairs.append((flat, int(np.ravel_multi_index([to[n] for n in names], sizes))))
    return pairs


def make_local(mesh):
    n_role, n_grp, n_tp = (mesh.shape[n] for n in ("role", "grp", "tp"))
    n_near = 2 if n_grp % 2 == 0 else 1
    n_far = n_grp // n_near
    xor_far = n_far & (n_far - 1) == 0
    names = mesh.axis_names

    def send(x, near=0, role=0, tp=0):
        return lax.ppermute(x, names, swap_table(mesh, lambda g: g ^ near, role, tp))

    def send_far(x, k):
        def grp_of(g):
            far, near = divmod(g, n_near)
            return (far ^ k if xor_far else (far + k) % n_far) * n_near + near

        return lax.ppermute(x, names, swap_table(mesh, grp_of, 0, 0))

    def local(
        q_new, k_new, v_new, k_cache, v_cache, cache_len, cycle_start, residual,
        out_proj, norm_gain, router, route_ids, w_gate, w_up, w_down,
    ):
        role, grp, tp = (lax.axis_index(n) for n in ("role", "grp", "tp"))
        tokens, quarter = residual.shape
        width = quarter * n_role * n_tp
        topk = route_ids.shape[1]
        experts = n_grp * w_gate.shape[0]
        cap = max(3, tokens * topk // experts + 2)
        far, near = grp // n_near, grp % n_near
        share = role * n_tp + tp
        heads_out = attend(q_new, k_new, v_new, k_cache, v_cache, cache_len, cycle_start)
        projected = jnp.dot(heads_out, out_proj, preferred_element_type=jnp.float32)
        blocks = projected.reshape(tokens, n_role, n_tp, quarter)

        def block(i, l):
            mine = lax.dynamic_index_in_dim(blocks, role ^ i, 1, keepdims=False)
            return lax.dynamic_index_in_dim(mine, tp ^ l, 1, keepdims=False)

        stream = residual.astype(jnp.float32) + block(0, 0)
        for i, l in ((1, 0), (1, 1), (0, 1)):
            stream = stream + send(block(i, l).astype(jnp.bfloat16), role=i, tp=l).astype(jnp.float32)
        attended = stream.astype(jnp.bfloat16)
        gain = lax.dynamic_slice_in_dim(norm_gain, share * quarter, quarter, 0)
        scaled = (stream * gain).astype(jnp.bfloat16)
        squares = jnp.sum(stream * stream, axis=1, keepdims=True)
        logits = jnp.dot(scaled, router, preferred_element_type=jnp.float32)
        named = route_ids[:, :, None] == jnp.arange(experts, dtype=jnp.int32)
        chosen = jnp.sum(jnp.where(named, logits[:, None, :], 0.0), axis=2)
        stats = split3(jnp.concatenate([squares, chosen], axis=1))
        packed = jnp.concatenate([scaled, route_ids.astype(jnp.bfloat16)] + stats, axis=1)
        lanes = -(-packed.shape[1] // 128) * 128
        packed = jnp.pad(packed, ((0, 0), (0, lanes - packed.shape[1])))
        gathered = jnp.stack([packed] + [send_far(packed, k) for k in range(1, n_far)])
        ids = gathered[:, :, quarter : quarter + topk].astype(jnp.float32)
        rows = {}
        selects = []
        for j in range(n_near):
            expert = (far * n_near + (near ^ j)).astype(jnp.float32)
            hit = jnp.sum((ids == expert).astype(jnp.int32), axis=2)
            rank = jnp.cumsum(hit, axis=1) - hit
            select = (hit[:, None, :] > 0) & (
                rank[:, None, :] == jnp.arange(cap, dtype=jnp.int32)[:, None]
            )
            select = select.astype(jnp.bfloat16)
            selects.append(select)
            rows[j] = jnp.einsum(
                "kct,ktw->kcw", select, gathered, preferred_element_type=jnp.float32
            ).astype(jnp.bfloat16).reshape(n_far * cap, lanes)
        arrived = {(0, 0): rows[0]}
        for j in range(n_near):
            for i in range(n_role):
                if (j, i) != (0, 0):
                    arrived[j, i] = send(rows[j], near=j, role=i)
        half = jnp.stack(
            [jnp.concatenate([arrived[j, i] for j in range(n_near)], 0) for i in range(n_role)]
        )
        other = send(half, tp=1)
        both = jnp.stack([half, other], 1)
        both = jnp.where(role == 0, both, both[::-1])
        both = jnp.where(tp == 0, both, both[:, ::-1])
        quarters = both.reshape(n_role * n_tp, -1, lanes)
        tail = jnp.sum(quarters[:, :, quarter + topk :].astype(jnp.float32), axis=0)
        own_ids = quarters[0, :, quarter : quarter + topk].astype(jnp.float32)
        n_stat = 1 + topk
        total = sum(tail[:, p * n_stat : (p + 1) * n_stat] for p in range(3))
        scale = lax.rsqrt(total[:, :1] / width + epsilon)
        picked = total[:, 1:] * scale
        lifted = jnp.exp(picked - jnp.max(picked, axis=1, keepdims=True))
        mine = jnp.where(own_ids == grp.astype(jnp.float32), lifted, 0.0)
        weight = jnp.sum(mine, axis=1, keepdims=True) / jnp.sum(lifted, axis=1, keepdims=True)
        inputs = jnp.concatenate([quarters[p, :, :quarter] for p in range(n_role * n_tp)], axis=1)
        gate_lin = jnp.dot(inputs, w_gate[0], preferred_element_type=jnp.float32) * scale
        up_lin = jnp.dot(inputs, w_up[0], preferred_element_type=jnp.float32) * scale
        activated = (gate_lin * jax.nn.sigmoid(1.702 * gate_lin) * (up_lin + 1.0)).astype(
            jnp.bfloat16
        )
        result = jnp.dot(activated, w_down[0], preferred_element_type=jnp.float32) * weight
        blocks_out = result.astype(jnp.bfloat16).reshape(-1, n_role, n_tp, quarter)
        blocks_out = jnp.where(role == 0, blocks_out, blocks_out[:, ::-1])
        blocks_out = jnp.where(tp == 0, blocks_out, blocks_out[:, :, ::-1])
        acc = blocks_out[:, :, 0].astype(jnp.float32) + send(blocks_out[:, :, 1], tp=1).astype(
            jnp.float32
        )
        acc = acc.astype(jnp.bfloat16).reshape(n_near, n_far * cap, n_role, quarter)
        back = []
        for j in range(n_near):
            total_rows = 0.0
            for i in range(n_role):
                piece = acc[j, :, i]
                if (j, i) != (0, 0):
                    piece = send(piece, near=j, role=i)
                total_rows = total_rows + piece.astype(jnp.float32)
            back.append(total_rows.astype(jnp.bfloat16).reshape(n_far, cap, quarter))
        spread = sum(
            jnp.einsum("kct,kcw->ktw", s, b, preferred_element_type=jnp.float32)
            for s, b in zip(selects, back)
        ).astype(jnp.bfloat16)
        mix = spread[0].astype(jnp.float32)
        for k in range(1, n_far):
            mix = mix + send_far(spread[k], k if xor_far else n_far - k).astype(jnp.float32)
        return (attended, mix.astype(jnp.bfloat16))

    return local


def solution(mesh):
    placed = (
        P("grp", ("role", "tp")),
        P("grp", ("role", "tp")),
        P("grp", ("role", "tp")),
        P("grp", None, ("role", "tp")),
        P("grp", None, ("role", "tp")),
        P("grp"),
        P("grp"),
        P("grp", ("role", "tp")),
        P(("role", "tp"), None),
        P(),
        P(("role", "tp"), None),
        P("grp", None),
        P("grp", None, ("role", "tp")),
        P("grp", None, ("role", "tp")),
        P("grp", ("role", "tp"), None),
    )
    return jax.shard_map(
        make_local(mesh),
        mesh=mesh,
        in_specs=placed,
        out_specs=(P("grp", ("role", "tp")), P("grp", ("role", "tp"))),
        check_vma=False,
    )
```

```python
import functools
import math

import jax
import jax.numpy as jnp
import numpy as np
from jax import lax
from jax.experimental import pallas as pl
from jax.experimental.pallas import tpu as pltpu
from jax.sharding import PartitionSpec as P

HEADS = 64
KV_HEADS = 8
HD = 64


epsilon = 1e-05


def attend_kernel(
    share_ref, len_hbm, start_hbm, q_hbm, kn_hbm, vn_hbm, k_hbm, v_hbm, wo_hbm,
    *rest, grouped, chunks, parts,
):
    outs, rest = rest[:parts], rest[parts:]
    len_ref, start_ref, q_ref, kn_ref, vn_ref, kbuf, vbuf, wobuf = rest[:8]
    queries, heads, small, ksem, vsem, wsem = rest[8:]
    tokens, window, lanes = k_hbm.shape
    pairs = (
        (q_hbm, q_ref), (kn_hbm, kn_ref), (vn_hbm, vn_ref), (len_hbm, len_ref),
        (start_hbm, start_ref),
    )
    firsts = [pltpu.make_async_copy(a, b, small.at[n]) for n, (a, b) in enumerate(pairs)]
    for copy in firsts:
        copy.start()
    n_heads = q_ref.shape[1] // HD
    step = tokens // chunks
    rows = wo_hbm.shape[0] // parts

    def kcopy(n):
        at = pl.ds(n * step, step)
        return pltpu.make_async_copy(k_hbm.at[at], kbuf.at[at], ksem.at[n])

    def vcopy(n):
        at = pl.ds(n * step, step)
        return pltpu.make_async_copy(v_hbm.at[at], vbuf.at[at], vsem.at[n])

    def wrows(k):
        return pl.ds(pl.multiple_of((share_ref[0] ^ k) * rows, 16), rows)

    def wcopy(k):
        return pltpu.make_async_copy(wo_hbm.at[wrows(k)], wobuf.at[wrows(k)], wsem.at[k])

    for n in range(chunks):
        kcopy(n).start()
        vcopy(n).start()
    for k in reversed(range(parts)):
        wcopy(k).start()
    for copy in firsts:
        copy.wait()
    lane = lax.broadcasted_iota(jnp.int32, (tokens, lanes), 1)
    per = lanes // HD

    def shifted(x, source, target):
        if source == target:
            return x
        return pltpu.roll(x, ((target - source) * HD) % lanes, 1)

    for h in range(n_heads):
        at = h // per * lanes
        x = q_ref[:, at : at + lanes].astype(jnp.float32)
        kv = h // grouped
        x = jnp.where(lane // HD == kv, shifted(x, h % per, kv), 0.0)
        queries[h * tokens : (h + 1) * tokens, :] = x
    factor = HD ** (-0.5)
    slots = lax.broadcasted_iota(jnp.int32, (1, window), 1)
    own_keys = kn_ref[...].astype(jnp.float32)
    own_values = vn_ref[...].astype(jnp.float32)
    for n in range(chunks):
        kcopy(n).wait()
        vcopy(n).wait()
        for t in range(n * step, (n + 1) * step):
            at = pl.ds(t, n_heads, stride=tokens)
            query = queries[at, :]
            scores = factor * lax.dot_general(
                query.astype(jnp.bfloat16), kbuf[t], (((1,), (1,)), ((), ())),
                preferred_element_type=jnp.float32,
            )
            own = factor * jnp.sum(query * own_keys[t : t + 1, :], axis=1, keepdims=True)
            age = slots - start_ref[t]
            age = jnp.where(age < 0, age + window, age)
            usable = age < len_ref[t]
            masked = jnp.where(usable, scores, -1e30)
            highest = jnp.maximum(jnp.max(masked, axis=1, keepdims=True), own)
            lifted = jnp.where(usable, jnp.exp(masked - highest), 0.0)
            own_lift = jnp.exp(own - highest)
            denominator = jnp.sum(lifted, axis=1, keepdims=True) + own_lift
            weights = (lifted / denominator).astype(jnp.bfloat16)
            own_weight = (own_lift / denominator).astype(jnp.bfloat16).astype(jnp.float32)
            mixed = jnp.dot(weights, vbuf[t], preferred_element_type=jnp.float32)
            heads[at, :] = mixed + own_weight * own_values[t : t + 1, :]
    columns = []
    for c in range(n_heads // per):
        column = None
        for p in range(per):
            h = c * per + p
            x = shifted(heads[h * tokens : (h + 1) * tokens, :], h // grouped, p)
            column = x if column is None else jnp.where(lane // HD == p, x, column)
        columns.append(column.astype(jnp.bfloat16))
    stacked = jnp.concatenate(columns, axis=1)
    for k in reversed(range(parts)):
        wcopy(k).wait()
        piece = lax.dot_general(
            stacked, wobuf[wrows(k), :], (((1,), (1,)), ((), ())),
            preferred_element_type=jnp.float32,
        )
        outs[k][...] = piece.astype(outs[k].dtype)


def attend_project(
    share, q_new, k_new, v_new, k_cache, v_cache, cache_len, cycle_start, out_proj, parts
):
    tokens, window, lanes = k_cache.shape
    n_heads = q_new.shape[1] // HD
    quarter = out_proj.shape[0] // parts
    chunks = 4
    smem = pl.BlockSpec(memory_space=pltpu.SMEM)
    vmem = pl.BlockSpec(memory_space=pltpu.VMEM)
    hbm = pl.BlockSpec(memory_space=pltpu.HBM)
    inputs = [
        pltpu.with_memory_space_constraint(x, pltpu.HBM)
        for x in (
            cache_len, cycle_start, q_new, k_new, v_new, k_cache, v_cache, out_proj
        )
    ]
    kinds = [jnp.float32] + [jnp.bfloat16] * (parts - 1)
    return pl.pallas_call(
        functools.partial(
            attend_kernel, grouped=HEADS // KV_HEADS, chunks=chunks, parts=parts
        ),
        in_specs=[smem] + [hbm] * 8,
        out_specs=[vmem] * parts,
        out_shape=[jax.ShapeDtypeStruct((tokens, quarter), kind) for kind in kinds],
        scratch_shapes=[
            pltpu.SMEM(cache_len.shape, jnp.int32),
            pltpu.SMEM(cycle_start.shape, jnp.int32),
            pltpu.VMEM(q_new.shape, q_new.dtype),
            pltpu.VMEM(k_new.shape, k_new.dtype),
            pltpu.VMEM(v_new.shape, v_new.dtype),
            pltpu.VMEM(k_cache.shape, k_cache.dtype),
            pltpu.VMEM(v_cache.shape, v_cache.dtype),
            pltpu.VMEM(out_proj.shape, out_proj.dtype),
            pltpu.VMEM((n_heads * tokens, lanes), jnp.float32),
            pltpu.VMEM((n_heads * tokens, lanes), jnp.float32),
            pltpu.SemaphoreType.DMA((5,)),
            pltpu.SemaphoreType.DMA((chunks,)),
            pltpu.SemaphoreType.DMA((chunks,)),
            pltpu.SemaphoreType.DMA((parts,)),
        ],
        compiler_params=pltpu.CompilerParams(vmem_limit_bytes=16 << 20),
        name="attend_project",
    )(share, *inputs)


def expert_kernel(
    place_ref, own_ref, other_ref, gate_ref, up_ref, down_ref, keep_ref, send_ref, pieces,
    *, quarter, topk,
):
    n_role, items, lanes = own_ref.shape
    n_tp = 2
    parts = n_role * n_tp
    share = place_ref[0]
    tail_at = quarter // 128 * 128
    first = quarter - tail_at
    tail = 0.0
    columns = []
    for p in range(parts):
        slot = share ^ p
        i, l = slot // n_tp, slot % n_tp
        x = jnp.where(l == 0, own_ref[i], other_ref[i])
        tail = tail + x[:, tail_at:].astype(jnp.float32)
        columns.append(x[:, :quarter])
    inputs = jnp.concatenate(columns, axis=1)
    turned = (((1,), (1,)), ((), ()))
    gate_lin = lax.dot_general(inputs, gate_ref[0], turned, preferred_element_type=jnp.float32)
    up_lin = lax.dot_general(inputs, up_ref[0], turned, preferred_element_type=jnp.float32)
    ids = own_ref[0, :, tail_at:].astype(jnp.float32)
    n_stat = 1 + topk

    def total(c):
        at = first + topk + c
        return sum(tail[:, at + p * n_stat : at + p * n_stat + 1] for p in range(3))

    scale = lax.rsqrt(total(0) / (parts * quarter) + epsilon)
    picked = [total(1 + k) * scale for k in range(topk)]
    top = functools.reduce(jnp.maximum, picked)
    lifted = [jnp.exp(x - top) for x in picked]
    expert = place_ref[1].astype(jnp.float32)
    mine = sum(
        jnp.where(ids[:, first + k : first + k + 1] == expert, lifted[k], 0.0)
        for k in range(topk)
    )
    weight = mine / sum(lifted)
    gate_lin = gate_lin * scale
    up_lin = up_lin * scale
    activated = gate_lin * jax.nn.sigmoid(1.702 * gate_lin) * (up_lin + 1.0)
    result = jnp.dot(
        activated.astype(jnp.bfloat16), down_ref[0], preferred_element_type=jnp.float32
    )
    result = result * weight
    for p in range(parts):
        pieces[p ^ share] = result[:, p * quarter : (p + 1) * quarter].astype(jnp.bfloat16)
    for i in range(n_role):
        keep_ref[i] = pieces[i * n_tp]
        send_ref[i] = pieces[i * n_tp + 1]


def run_expert(place, own, other, w_gate, w_up, w_down, quarter, topk):
    n_role, items, _ = own.shape
    smem = pl.BlockSpec(memory_space=pltpu.SMEM)
    vmem = pl.BlockSpec(memory_space=pltpu.VMEM)
    shape = jax.ShapeDtypeStruct((n_role, items, quarter), jnp.bfloat16)
    return pl.pallas_call(
        functools.partial(expert_kernel, quarter=quarter, topk=topk),
        in_specs=[smem] + [vmem] * 5,
        out_specs=[vmem, vmem],
        out_shape=[shape, shape],
        scratch_shapes=[pltpu.VMEM((2 * n_role, items, quarter), jnp.bfloat16)],
        compiler_params=pltpu.CompilerParams(vmem_limit_bytes=24 << 20),
        name="expert",
    )(place, own, other, w_gate, w_up, w_down)


def split3(x):
    high = lax.reduce_precision(x, 8, 7)
    rest = x - high
    middle = lax.reduce_precision(rest, 8, 7)
    low = rest - middle
    return [part.astype(jnp.bfloat16) for part in (high, middle, low)]


def swap_table(mesh, grp_of, role_flip, tp_flip):
    names = mesh.axis_names
    sizes = [mesh.shape[n] for n in names]
    pairs = []
    for flat in range(math.prod(sizes)):
        at = dict(zip(names, [int(v) for v in np.unravel_index(flat, sizes)]))
        to = dict(
            role=at["role"] ^ role_flip, tp=at["tp"] ^ tp_flip, grp=grp_of(at["grp"])
        )
        pairs.append((flat, int(np.ravel_multi_index([to[n] for n in names], sizes))))
    return pairs


def make_local(mesh):
    n_role, n_grp, n_tp = (mesh.shape[n] for n in ("role", "grp", "tp"))
    n_near = 2 if n_grp % 2 == 0 else 1
    n_far = n_grp // n_near
    xor_far = n_far & (n_far - 1) == 0
    names = mesh.axis_names

    def send(x, near=0, role=0, tp=0):
        return lax.ppermute(x, names, swap_table(mesh, lambda g: g ^ near, role, tp))

    def send_far(x, k):
        def grp_of(g):
            far, near = divmod(g, n_near)
            return (far ^ k if xor_far else (far + k) % n_far) * n_near + near

        return lax.ppermute(x, names, swap_table(mesh, grp_of, 0, 0))

    def local(
        q_new, k_new, v_new, k_cache, v_cache, cache_len, cycle_start, residual,
        out_proj, norm_gain, router, route_ids, w_gate, w_up, w_down,
    ):
        role, grp, tp = (lax.axis_index(n) for n in ("role", "grp", "tp"))
        tokens, quarter = residual.shape
        width = quarter * n_role * n_tp
        topk = route_ids.shape[1]
        experts = n_grp * w_gate.shape[0]
        cap = max(3, tokens * topk // experts + 2)
        far, near = grp // n_near, grp % n_near
        share = role * n_tp + tp
        parts = n_role * n_tp
        place = share.astype(jnp.int32).reshape(1)
        pieces = attend_project(
            place, q_new, k_new, v_new, k_cache, v_cache, cache_len, cycle_start, out_proj.T, parts
        )
        stream = residual.astype(jnp.float32) + pieces[0]
        for k in (2, 3, 1):
            moved = send(pieces[k], role=k // n_tp, tp=k % n_tp)
            stream = stream + moved.astype(jnp.float32)
        attended = stream.astype(jnp.bfloat16)
        gain = lax.dynamic_slice_in_dim(norm_gain, share * quarter, quarter, 0)
        scaled = (stream * gain).astype(jnp.bfloat16)
        squares = jnp.sum(stream * stream, axis=1, keepdims=True)
        logits = jnp.dot(scaled, router, preferred_element_type=jnp.float32)
        named = route_ids[:, :, None] == jnp.arange(experts, dtype=jnp.int32)
        chosen = jnp.sum(jnp.where(named, logits[:, None, :], 0.0), axis=2)
        stats = split3(jnp.concatenate([squares, chosen], axis=1))
        packed = jnp.concatenate([scaled, route_ids.astype(jnp.bfloat16)] + stats, axis=1)
        lanes = -(-packed.shape[1] // 128) * 128
        packed = jnp.pad(packed, ((0, 0), (0, lanes - packed.shape[1])))
        gathered = jnp.stack([packed] + [send_far(packed, k) for k in range(1, n_far)])
        ids = gathered[:, :, quarter : quarter + topk].astype(jnp.float32)
        rows = {}
        selects = []
        for j in range(n_near):
            expert = (far * n_near + (near ^ j)).astype(jnp.float32)
            hit = jnp.sum((ids == expert).astype(jnp.int32), axis=2)
            rank = jnp.cumsum(hit, axis=1) - hit
            select = (hit[:, None, :] > 0) & (
                rank[:, None, :] == jnp.arange(cap, dtype=jnp.int32)[:, None]
            )
            select = select.astype(jnp.bfloat16)
            selects.append(select)
            rows[j] = jnp.einsum(
                "kct,ktw->kcw", select, gathered, preferred_element_type=jnp.float32
            ).astype(jnp.bfloat16).reshape(n_far * cap, lanes)
        arrived = {(0, 0): rows[0]}
        for j in range(n_near):
            for i in range(n_role):
                if (j, i) != (0, 0):
                    arrived[j, i] = send(rows[j], near=j, role=i)
        half = jnp.stack(
            [jnp.concatenate([arrived[j, i] for j in range(n_near)], 0) for i in range(n_role)]
        )
        other = send(half, tp=1)
        place = jnp.stack([share, grp]).astype(jnp.int32)
        kept, sent = run_expert(
            place, half, other, jnp.swapaxes(w_gate, 1, 2), jnp.swapaxes(w_up, 1, 2), w_down,
            quarter, topk,
        )
        acc = kept.astype(jnp.float32) + send(sent, tp=1).astype(jnp.float32)
        acc = acc.astype(jnp.bfloat16).reshape(n_role, n_near, n_far * cap, quarter)
        back = []
        for j in range(n_near):
            total_rows = 0.0
            for i in range(n_role):
                piece = acc[i, j]
                if (j, i) != (0, 0):
                    piece = send(piece, near=j, role=i)
                total_rows = total_rows + piece.astype(jnp.float32)
            back.append(total_rows.astype(jnp.bfloat16).reshape(n_far, cap, quarter))
        spread = sum(
            jnp.einsum("kct,kcw->ktw", s, b, preferred_element_type=jnp.float32)
            for s, b in zip(selects, back)
        ).astype(jnp.bfloat16)
        mix = spread[0].astype(jnp.float32)
        for k in range(1, n_far):
            mix = mix + send_far(spread[k], k if xor_far else n_far - k).astype(jnp.float32)
        return (attended, mix.astype(jnp.bfloat16))

    return local


def solution(mesh):
    placed = (
        P("grp", ("role", "tp")),
        P("grp", ("role", "tp")),
        P("grp", ("role", "tp")),
        P("grp", None, ("role", "tp")),
        P("grp", None, ("role", "tp")),
        P("grp"),
        P("grp"),
        P("grp", ("role", "tp")),
        P(("role", "tp"), None),
        P(),
        P(("role", "tp"), None),
        P("grp", None),
        P("grp", None, ("role", "tp")),
        P("grp", None, ("role", "tp")),
        P("grp", ("role", "tp"), None),
    )
    return jax.shard_map(
        make_local(mesh),
        mesh=mesh,
        in_specs=placed,
        out_specs=(P("grp", ("role", "tp")), P("grp", ("role", "tp"))),
        check_vma=False,
    )
```

```python
import functools
import math

import jax
import jax.numpy as jnp
import numpy as np
from jax import lax
from jax.experimental import pallas as pl
from jax.experimental.pallas import tpu as pltpu
from jax.sharding import PartitionSpec as P

HEADS = 64
KV_HEADS = 8
HD = 64


epsilon = 1e-05
COVER = 1 << 33


def attend_kernel(
    share_ref, len_hbm, start_hbm, q_hbm, kn_hbm, vn_hbm, k_hbm, v_hbm, wo_hbm,
    *rest, grouped, chunks, parts,
):
    outs, rest = rest[:parts], rest[parts:]
    len_ref, start_ref, q_ref, kn_ref, vn_ref, kbuf, vbuf, wobuf = rest[:8]
    queries, heads, scores, products, small, ksem, vsem, wsem = rest[8:]
    tokens, window, lanes = k_hbm.shape
    pairs = (
        (q_hbm, q_ref), (kn_hbm, kn_ref), (vn_hbm, vn_ref), (len_hbm, len_ref),
        (start_hbm, start_ref),
    )
    firsts = [pltpu.make_async_copy(a, b, small.at[n]) for n, (a, b) in enumerate(pairs)]
    for copy in firsts:
        copy.start()
    n_heads = q_ref.shape[1] // HD
    step = tokens // chunks
    rows = wo_hbm.shape[0] // parts

    def kcopy(n):
        at = pl.ds(n * step, step)
        return pltpu.make_async_copy(k_hbm.at[at], kbuf.at[at], ksem.at[n])

    def vcopy(n):
        at = pl.ds(n * step, step)
        return pltpu.make_async_copy(v_hbm.at[at], vbuf.at[at], vsem.at[n])

    def wrows(k):
        return pl.ds(pl.multiple_of((share_ref[0] ^ k) * rows, 16), rows)

    def wcopy(k):
        return pltpu.make_async_copy(wo_hbm.at[wrows(k)], wobuf.at[wrows(k)], wsem.at[k])

    for n in range(chunks):
        kcopy(n).start()
        vcopy(n).start()
    for k in reversed(range(parts)):
        wcopy(k).start()
    for copy in firsts:
        copy.wait()
    lane = lax.broadcasted_iota(jnp.int32, (tokens, lanes), 1)
    per = lanes // HD

    def shifted(x, source, target):
        if source == target:
            return x
        return pltpu.roll(x, ((target - source) * HD) % lanes, 1)

    for h in range(n_heads):
        at = h // per * lanes
        x = q_ref[:, at : at + lanes].astype(jnp.float32)
        kv = h // grouped
        x = jnp.where(lane // HD == kv, shifted(x, h % per, kv), 0.0)
        queries[h * tokens : (h + 1) * tokens, :] = x
    factor = HD ** (-0.5)
    slots = lax.broadcasted_iota(jnp.int32, (1, window), 1)
    own_keys = kn_ref[...].astype(jnp.float32)
    own_values = vn_ref[...].astype(jnp.float32)
    block = step * n_heads
    for n in range(chunks):
        kcopy(n).wait()
        for t in range(n * step, (n + 1) * step):
            query = queries[pl.ds(t, n_heads, stride=tokens), :]
            dots = lax.dot_general(
                query.astype(jnp.bfloat16), kbuf[t], (((1,), (1,)), ((), ())),
                preferred_element_type=jnp.float32,
            )
            age = slots - start_ref[t]
            age = jnp.where(age < 0, age + window, age)
            at = pl.ds(t * n_heads, n_heads)
            scores[at, :] = jnp.where(age < len_ref[t], factor * dots, -1e30)
            products[at, :] = query * own_keys[t : t + 1, :]
    for n in range(chunks):
        at = pl.ds(n * block, block)
        masked = scores[at, :]
        own = factor * jnp.sum(products[at, :], axis=1, keepdims=True)
        highest = jnp.maximum(jnp.max(masked, axis=1, keepdims=True), own)
        lifted = jnp.exp(masked - highest)
        own_lift = jnp.exp(own - highest)
        denominator = jnp.sum(lifted, axis=1, keepdims=True) + own_lift
        weights = (lifted / denominator).astype(jnp.bfloat16)
        own_weight = (own_lift / denominator).astype(jnp.bfloat16).astype(jnp.float32)
        vcopy(n).wait()
        for m in range(step):
            t = n * step + m
            mine = slice(m * n_heads, (m + 1) * n_heads)
            mixed = jnp.dot(weights[mine], vbuf[t], preferred_element_type=jnp.float32)
            mixed = mixed + own_weight[mine] * own_values[t : t + 1, :]
            heads[pl.ds(t, n_heads, stride=tokens), :] = mixed
    columns = []
    for c in range(n_heads // per):
        column = None
        for p in range(per):
            h = c * per + p
            x = shifted(heads[h * tokens : (h + 1) * tokens, :], h // grouped, p)
            column = x if column is None else jnp.where(lane // HD == p, x, column)
        columns.append(column.astype(jnp.bfloat16))
    stacked = jnp.concatenate(columns, axis=1)
    for k in reversed(range(parts)):
        wcopy(k).wait()
        piece = lax.dot_general(
            stacked, wobuf[wrows(k), :], (((1,), (1,)), ((), ())),
            preferred_element_type=jnp.float32,
        )
        outs[k][...] = piece.astype(outs[k].dtype)


def attend_project(
    share, q_new, k_new, v_new, k_cache, v_cache, cache_len, cycle_start, out_proj, parts
):
    tokens, window, lanes = k_cache.shape
    n_heads = q_new.shape[1] // HD
    quarter = out_proj.shape[0] // parts
    chunks = 4
    smem = pl.BlockSpec(memory_space=pltpu.SMEM)
    vmem = pl.BlockSpec(memory_space=pltpu.VMEM)
    hbm = pl.BlockSpec(memory_space=pltpu.HBM)
    inputs = [
        pltpu.with_memory_space_constraint(x, pltpu.HBM)
        for x in (
            cache_len, cycle_start, q_new, k_new, v_new, k_cache, v_cache, out_proj
        )
    ]
    kinds = [jnp.float32] + [jnp.bfloat16] * (parts - 1)
    return pl.pallas_call(
        functools.partial(
            attend_kernel, grouped=HEADS // KV_HEADS, chunks=chunks, parts=parts
        ),
        in_specs=[smem] + [hbm] * 8,
        out_specs=[vmem] * parts,
        out_shape=[jax.ShapeDtypeStruct((tokens, quarter), kind) for kind in kinds],
        scratch_shapes=[
            pltpu.SMEM(cache_len.shape, jnp.int32),
            pltpu.SMEM(cycle_start.shape, jnp.int32),
            pltpu.VMEM(q_new.shape, q_new.dtype),
            pltpu.VMEM(k_new.shape, k_new.dtype),
            pltpu.VMEM(v_new.shape, v_new.dtype),
            pltpu.VMEM(k_cache.shape, k_cache.dtype),
            pltpu.VMEM(v_cache.shape, v_cache.dtype),
            pltpu.VMEM(out_proj.shape, out_proj.dtype),
            pltpu.VMEM((n_heads * tokens, lanes), jnp.float32),
            pltpu.VMEM((n_heads * tokens, lanes), jnp.float32),
            pltpu.VMEM((n_heads * tokens, window), jnp.float32),
            pltpu.VMEM((n_heads * tokens, lanes), jnp.float32),
            pltpu.SemaphoreType.DMA((5,)),
            pltpu.SemaphoreType.DMA((chunks,)),
            pltpu.SemaphoreType.DMA((chunks,)),
            pltpu.SemaphoreType.DMA((parts,)),
        ],
        compiler_params=pltpu.CompilerParams(vmem_limit_bytes=16 << 20),
        name="attend_project",
    )(share, *inputs)


def expert_kernel(
    place_ref, own_ref, other_ref, gate_ref, up_ref, down_ref, keep_ref, send_ref, pieces,
    *, quarter, topk,
):
    n_role, items, lanes = own_ref.shape
    n_tp = 2
    parts = n_role * n_tp
    share = place_ref[0]
    tail_at = quarter // 128 * 128
    first = quarter - tail_at
    tail = 0.0
    columns = []
    for p in range(parts):
        slot = share ^ p
        i, l = slot // n_tp, slot % n_tp
        x = jnp.where(l == 0, own_ref[i], other_ref[i])
        tail = tail + x[:, tail_at:].astype(jnp.float32)
        columns.append(x[:, :quarter])
    inputs = jnp.concatenate(columns, axis=1)
    turned = (((1,), (1,)), ((), ()))
    gate_lin = lax.dot_general(inputs, gate_ref[0], turned, preferred_element_type=jnp.float32)
    up_lin = lax.dot_general(inputs, up_ref[0], turned, preferred_element_type=jnp.float32)
    ids = own_ref[0, :, tail_at:].astype(jnp.float32)
    n_stat = 1 + topk

    def total(c):
        at = first + topk + c
        return sum(tail[:, at + p * n_stat : at + p * n_stat + 1] for p in range(3))

    scale = lax.rsqrt(total(0) / (parts * quarter) + epsilon)
    picked = [total(1 + k) * scale for k in range(topk)]
    top = functools.reduce(jnp.maximum, picked)
    lifted = [jnp.exp(x - top) for x in picked]
    expert = place_ref[1].astype(jnp.float32)
    mine = sum(
        jnp.where(ids[:, first + k : first + k + 1] == expert, lifted[k], 0.0)
        for k in range(topk)
    )
    weight = mine / sum(lifted)
    gate_lin = gate_lin * scale
    up_lin = up_lin * scale
    activated = gate_lin * jax.nn.sigmoid(1.702 * gate_lin) * (up_lin + 1.0)
    result = jnp.dot(
        activated.astype(jnp.bfloat16), down_ref[0], preferred_element_type=jnp.float32
    )
    result = result * weight
    for p in range(parts):
        pieces[p ^ share] = result[:, p * quarter : (p + 1) * quarter].astype(jnp.bfloat16)
    for i in range(n_role):
        keep_ref[i] = pieces[i * n_tp]
        send_ref[i] = pieces[i * n_tp + 1]


def run_expert(place, own, other, w_gate, w_up, w_down, quarter, topk):
    n_role, items, _ = own.shape
    smem = pl.BlockSpec(memory_space=pltpu.SMEM)
    vmem = pl.BlockSpec(memory_space=pltpu.VMEM)
    shape = jax.ShapeDtypeStruct((n_role, items, quarter), jnp.bfloat16)
    return pl.pallas_call(
        functools.partial(expert_kernel, quarter=quarter, topk=topk),
        in_specs=[smem] + [vmem] * 5,
        out_specs=[vmem, vmem],
        out_shape=[shape, shape],
        scratch_shapes=[pltpu.VMEM((2 * n_role, items, quarter), jnp.bfloat16)],
        compiler_params=pltpu.CompilerParams(vmem_limit_bytes=24 << 20),
        name="expert",
    )(place, own, other, w_gate, w_up, w_down)


def three_parts(x):
    high = x.astype(jnp.bfloat16).astype(jnp.float32)
    rest = x - high
    middle = rest.astype(jnp.bfloat16).astype(jnp.float32)
    return high, middle, rest - middle


def pack_kernel(own_ref, *rest, moved):
    arrived, rest = rest[:moved], rest[moved:]
    residual_ref, gain_ref, router_ref, ids_ref, attended_ref, packed_ref = rest
    stream = residual_ref[...].astype(jnp.float32) + own_ref[...]
    for ref in arrived:
        stream = stream + ref[...].astype(jnp.float32)
    attended_ref[...] = stream.astype(jnp.bfloat16)
    tokens, quarter = stream.shape
    topk = ids_ref.shape[0]
    scaled = (stream * gain_ref[...]).astype(jnp.bfloat16)
    squares = jnp.sum(stream * stream, axis=1, keepdims=True)
    logits = lax.dot_general(
        scaled, router_ref[...], (((1,), (1,)), ((), ())), preferred_element_type=jnp.float32
    )
    names = lax.broadcasted_iota(jnp.int32, logits.shape, 1).astype(jnp.float32)
    eye = (
        lax.broadcasted_iota(jnp.int32, (topk, topk), 0)
        == lax.broadcasted_iota(jnp.int32, (topk, topk), 1)
    )
    ids = lax.dot_general(
        ids_ref[...].astype(jnp.float32).astype(jnp.bfloat16), eye.astype(jnp.bfloat16),
        (((0,), (0,)), ((), ())), preferred_element_type=jnp.float32,
    )
    stats = [squares]
    columns = []
    for k in range(topk):
        chosen = ids[:, k : k + 1]
        columns.append(chosen)
        stats.append(jnp.sum(jnp.where(names == chosen, logits, 0.0), axis=1, keepdims=True))
    split = [three_parts(x) for x in stats]
    for p in range(3):
        columns.extend(x[p] for x in split)
    tail_at = quarter // 128 * 128
    first = quarter - tail_at
    packed_ref[:, :quarter] = scaled
    tile = packed_ref[:, tail_at : tail_at + 128]
    lane = lax.broadcasted_iota(jnp.int32, (tokens, 128), 1)
    tail = jnp.zeros((tokens, 128), jnp.float32)
    for c, x in enumerate(columns):
        tail = jnp.where(lane == first + c, x, tail)
    packed_ref[:, tail_at : tail_at + 128] = jnp.where(
        lane < first, tile.astype(jnp.float32), tail
    ).astype(jnp.bfloat16)


def run_pack(own, arrived, residual, gain, router, route_ids):
    tokens, quarter = residual.shape
    vmem = pl.BlockSpec(memory_space=pltpu.VMEM)
    lanes = quarter // 128 * 128 + 128
    assert quarter % 128 + 4 * route_ids.shape[0] + 3 <= 128
    return pl.pallas_call(
        functools.partial(pack_kernel, moved=len(arrived)),
        in_specs=[vmem] * (5 + len(arrived)),
        out_specs=[vmem, vmem],
        out_shape=[
            jax.ShapeDtypeStruct((tokens, quarter), jnp.bfloat16),
            jax.ShapeDtypeStruct((tokens, lanes), jnp.bfloat16),
        ],
        compiler_params=pltpu.CompilerParams(vmem_limit_bytes=4 << 20),
        cost_estimate=pl.CostEstimate(flops=COVER, transcendentals=0, bytes_accessed=1 << 20),
        name="pack",
    )(own, *arrived, residual, gain, router, route_ids)


def select_kernel(expert_ref, *rest, n_far, n_near, cap, topk, quarter):
    blocks, rest = rest[:n_far], rest[n_far:]
    rows, picks = rest[:n_near], rest[n_near:]
    tokens, lanes = blocks[0].shape
    tail_at = quarter // 128 * 128
    first = quarter - tail_at
    stacked = jnp.concatenate([ref[...] for ref in blocks], axis=0)
    ids = stacked[:, tail_at:].astype(jnp.float32)
    n_all = n_far * tokens
    down = lax.broadcasted_iota(jnp.int32, (tokens, tokens), 0)
    across = lax.broadcasted_iota(jnp.int32, (tokens, tokens), 1)
    before = (across < down).astype(jnp.bfloat16)
    slot = lax.broadcasted_iota(jnp.int32, (n_all, n_far * cap), 1).astype(jnp.float32)
    base = (lax.broadcasted_iota(jnp.int32, (n_all, 1), 0) // tokens * cap).astype(jnp.float32)
    hits = []
    for j in range(n_near):
        expert = expert_ref[j].astype(jnp.float32)
        hit = jnp.zeros((n_all, 1), jnp.float32)
        for k in range(topk):
            hit = hit + jnp.where(ids[:, first + k : first + k + 1] == expert, 1.0, 0.0)
        hits.append(hit)
    lane = lax.broadcasted_iota(jnp.int32, (n_all, 128), 1)
    table = jnp.zeros((n_all, 128), jnp.float32)
    for j in range(n_near):
        table = jnp.where(lane == j, hits[j], table)
    table = table.astype(jnp.bfloat16)
    ranks = jnp.concatenate(
        [
            jnp.dot(
                before, table[n * tokens : (n + 1) * tokens], preferred_element_type=jnp.float32
            )
            for n in range(n_far)
        ],
        axis=0,
    )
    for j in range(n_near):
        at = jnp.where(hits[j] > 0.0, ranks[:, j : j + 1] + base, -1.0)
        pick = jnp.where(at == slot, 1.0, 0.0).astype(jnp.bfloat16)
        picks[j][...] = pick
        rows[j][...] = lax.dot_general(
            pick, stacked, (((0,), (0,)), ((), ())), preferred_element_type=jnp.float32
        ).astype(jnp.bfloat16)


def run_select(experts, blocks, n_near, cap, topk, quarter):
    tokens, lanes = blocks[0].shape
    n_far = len(blocks)
    vmem = pl.BlockSpec(memory_space=pltpu.VMEM)
    outs = [jax.ShapeDtypeStruct((n_far * cap, lanes), jnp.bfloat16)] * n_near
    outs += [jax.ShapeDtypeStruct((n_far * tokens, n_far * cap), jnp.bfloat16)] * n_near
    made = pl.pallas_call(
        functools.partial(
            select_kernel, n_far=n_far, n_near=n_near, cap=cap, topk=topk, quarter=quarter
        ),
        in_specs=[pl.BlockSpec(memory_space=pltpu.SMEM)] + [vmem] * n_far,
        out_specs=[vmem] * len(outs),
        out_shape=outs,
        compiler_params=pltpu.CompilerParams(vmem_limit_bytes=12 << 20),
        name="select",
    )(experts, *blocks)
    return made[:n_near], made[n_near:]


def spread_kernel(*refs, n_near, n_role, n_far):
    rows, refs = refs[: n_near * n_role], refs[n_near * n_role :]
    picks, outs = refs[:n_near], refs[n_near:]
    total = 0.0
    for j in range(n_near):
        row = 0.0
        for i in range(n_role):
            row = row + rows[j * n_role + i][...].astype(jnp.float32)
        total = total + jnp.dot(
            picks[j][...], row.astype(jnp.bfloat16), preferred_element_type=jnp.float32
        )
    tokens = total.shape[0] // n_far
    for n in range(n_far):
        outs[n][...] = total[n * tokens : (n + 1) * tokens].astype(outs[n].dtype)


def run_spread(rows, picks, n_role, n_far):
    n_near = len(picks)
    tokens = picks[0].shape[0] // n_far
    vmem = pl.BlockSpec(memory_space=pltpu.VMEM)
    quarter = rows[0].shape[1]
    kinds = [jnp.float32] + [jnp.bfloat16] * (n_far - 1)
    return pl.pallas_call(
        functools.partial(spread_kernel, n_near=n_near, n_role=n_role, n_far=n_far),
        in_specs=[vmem] * (len(rows) + n_near),
        out_specs=[vmem] * n_far,
        out_shape=[jax.ShapeDtypeStruct((tokens, quarter), kind) for kind in kinds],
        compiler_params=pltpu.CompilerParams(vmem_limit_bytes=12 << 20),
        name="spread",
    )(*rows, *picks)


def swap_table(mesh, grp_of, role_flip, tp_flip):
    names = mesh.axis_names
    sizes = [mesh.shape[n] for n in names]
    pairs = []
    for flat in range(math.prod(sizes)):
        at = dict(zip(names, [int(v) for v in np.unravel_index(flat, sizes)]))
        to = dict(
            role=at["role"] ^ role_flip, tp=at["tp"] ^ tp_flip, grp=grp_of(at["grp"])
        )
        pairs.append((flat, int(np.ravel_multi_index([to[n] for n in names], sizes))))
    return pairs


def make_local(mesh):
    n_role, n_grp, n_tp = (mesh.shape[n] for n in ("role", "grp", "tp"))
    n_near = 2 if n_grp % 2 == 0 else 1
    n_far = n_grp // n_near
    xor_far = n_far & (n_far - 1) == 0
    names = mesh.axis_names

    def send(x, near=0, role=0, tp=0):
        return lax.ppermute(x, names, swap_table(mesh, lambda g: g ^ near, role, tp))

    def send_far(x, k):
        def grp_of(g):
            far, near = divmod(g, n_near)
            return (far ^ k if xor_far else (far + k) % n_far) * n_near + near

        return lax.ppermute(x, names, swap_table(mesh, grp_of, 0, 0))

    def local(
        q_new, k_new, v_new, k_cache, v_cache, cache_len, cycle_start, residual,
        out_proj, norm_gain, router, route_ids, w_gate, w_up, w_down,
    ):
        role, grp, tp = (lax.axis_index(n) for n in ("role", "grp", "tp"))
        tokens, quarter = residual.shape
        width = quarter * n_role * n_tp
        topk = route_ids.shape[1]
        experts = n_grp * w_gate.shape[0]
        cap = max(3, tokens * topk // experts + 2)
        far, near = grp // n_near, grp % n_near
        share = role * n_tp + tp
        parts = n_role * n_tp
        place = share.astype(jnp.int32).reshape(1)
        pieces = attend_project(
            place, q_new, k_new, v_new, k_cache, v_cache, cache_len, cycle_start, out_proj.T, parts
        )
        moved = [send(pieces[k], role=k // n_tp, tp=k % n_tp) for k in range(1, parts)]
        gain = lax.dynamic_slice_in_dim(norm_gain, share * quarter, quarter, 0).reshape(1, quarter)
        attended, packed = run_pack(pieces[0], moved, residual, gain, router.T, route_ids.T)
        blocks = [packed] + [send_far(packed, k) for k in range(1, n_far)]
        experts_near = jnp.stack([far * n_near + (near ^ j) for j in range(n_near)])
        rows, picks = run_select(
            experts_near.astype(jnp.int32), blocks, n_near, cap, topk, quarter
        )
        arrived = {(0, 0): rows[0]}
        for j in range(n_near):
            for i in range(n_role):
                if (j, i) != (0, 0):
                    arrived[j, i] = send(rows[j], near=j, role=i)
        half = jnp.stack(
            [jnp.concatenate([arrived[j, i] for j in range(n_near)], 0) for i in range(n_role)]
        )
        other = send(half, tp=1)
        place = jnp.stack([share, grp]).astype(jnp.int32)
        kept, sent = run_expert(
            place, half, other, jnp.swapaxes(w_gate, 1, 2), jnp.swapaxes(w_up, 1, 2), w_down,
            quarter, topk,
        )
        acc = kept.astype(jnp.float32) + send(sent, tp=1).astype(jnp.float32)
        acc = acc.astype(jnp.bfloat16).reshape(n_role, n_near, n_far * cap, quarter)
        back = []
        for j in range(n_near):
            for i in range(n_role):
                piece = acc[i, j]
                if (j, i) != (0, 0):
                    piece = send(piece, near=j, role=i)
                back.append(piece)
        spread = run_spread(back, picks, n_role, n_far)
        mix = spread[0].astype(jnp.float32)
        for k in range(1, n_far):
            mix = mix + send_far(spread[k], k if xor_far else n_far - k).astype(jnp.float32)
        return (attended, mix.astype(jnp.bfloat16))

    return local


def solution(mesh):
    placed = (
        P("grp", ("role", "tp")),
        P("grp", ("role", "tp")),
        P("grp", ("role", "tp")),
        P("grp", None, ("role", "tp")),
        P("grp", None, ("role", "tp")),
        P("grp"),
        P("grp"),
        P("grp", ("role", "tp")),
        P(("role", "tp"), None),
        P(),
        P(("role", "tp"), None),
        P("grp", None),
        P("grp", None, ("role", "tp")),
        P("grp", None, ("role", "tp")),
        P("grp", ("role", "tp"), None),
    )
    return jax.shard_map(
        make_local(mesh),
        mesh=mesh,
        in_specs=placed,
        out_specs=(P("grp", ("role", "tp")), P("grp", ("role", "tp"))),
        check_vma=False,
    )
```

```python
import functools
import math

import jax
import jax.numpy as jnp
import numpy as np
from jax import lax
from jax.experimental import pallas as pl
from jax.experimental.pallas import tpu as pltpu
from jax.sharding import PartitionSpec as P


HEADS = 64
KV_HEADS = 8
HD = 64


epsilon = 1e-05
COVER = 1 << 33


def attend_kernel(
    share_ref, len_hbm, start_hbm, q_hbm, kn_hbm, vn_hbm, k_hbm, v_hbm, wo_hbm,
    *rest, grouped, chunks, parts,
):
    early = parts // 2
    outs, (stacked_ref, later_ref), rest = rest[:early], rest[early : early + 2], rest[early + 2 :]
    len_ref, start_ref, q_ref, kn_ref, vn_ref, kbuf, vbuf, wobuf = rest[:8]
    queries, heads, scores, products, small, ksem, vsem, wsem = rest[8:]
    tokens, window, lanes = k_hbm.shape
    pairs = (
        (q_hbm, q_ref), (kn_hbm, kn_ref), (vn_hbm, vn_ref), (len_hbm, len_ref),
        (start_hbm, start_ref),
    )
    firsts = [pltpu.make_async_copy(a, b, small.at[n]) for n, (a, b) in enumerate(pairs)]
    for copy in firsts:
        copy.start()
    n_heads = q_ref.shape[1] // HD
    step = tokens // chunks
    rows = wo_hbm.shape[0] // parts

    def kcopy(n):
        at = pl.ds(n * step, step)
        return pltpu.make_async_copy(k_hbm.at[at], kbuf.at[at], ksem.at[n])

    def vcopy(n):
        at = pl.ds(n * step, step)
        return pltpu.make_async_copy(v_hbm.at[at], vbuf.at[at], vsem.at[n])

    def wrows(k):
        return pl.ds(pl.multiple_of((share_ref[0] ^ k) * rows, 16), rows)

    def wcopy(k):
        target = wobuf.at[k - early] if k >= early else later_ref.at[k]
        return pltpu.make_async_copy(wo_hbm.at[wrows(k)], target, wsem.at[k])

    for n in range(chunks):
        kcopy(n).start()
        vcopy(n).start()
    for copy in firsts:
        copy.wait()
    lane = lax.broadcasted_iota(jnp.int32, (tokens, lanes), 1)
    per = lanes // HD

    def shifted(x, source, target):
        if source == target:
            return x
        return pltpu.roll(x, ((target - source) * HD) % lanes, 1)

    for h in range(n_heads):
        at = h // per * lanes
        x = q_ref[:, at : at + lanes].astype(jnp.float32)
        kv = h // grouped
        x = jnp.where(lane // HD == kv, shifted(x, h % per, kv), 0.0)
        queries[h * tokens : (h + 1) * tokens, :] = x
    factor = HD ** (-0.5)
    slots = lax.broadcasted_iota(jnp.int32, (1, window), 1)
    own_keys = kn_ref[...].astype(jnp.float32)
    own_values = vn_ref[...].astype(jnp.float32)
    block = step * n_heads
    for n in range(chunks):
        kcopy(n).wait()
        if n == 0:
            for k in reversed(range(parts)):
                wcopy(k).start()
        for t in range(n * step, (n + 1) * step):
            query = queries[pl.ds(t, n_heads, stride=tokens), :]
            dots = lax.dot_general(
                query.astype(jnp.bfloat16), kbuf[t], (((1,), (1,)), ((), ())),
                preferred_element_type=jnp.float32,
            )
            age = slots - start_ref[t]
            age = jnp.where(age < 0, age + window, age)
            at = pl.ds(t * n_heads, n_heads)
            scores[at, :] = jnp.where(age < len_ref[t], factor * dots, -1e30)
            products[at, :] = query * own_keys[t : t + 1, :]
    for n in range(chunks):
        at = pl.ds(n * block, block)
        masked = scores[at, :]
        own = factor * jnp.sum(products[at, :], axis=1, keepdims=True)
        highest = jnp.maximum(jnp.max(masked, axis=1, keepdims=True), own)
        lifted = jnp.exp(masked - highest)
        own_lift = jnp.exp(own - highest)
        denominator = jnp.sum(lifted, axis=1, keepdims=True) + own_lift
        weights = (lifted / denominator).astype(jnp.bfloat16)
        own_weight = (own_lift / denominator).astype(jnp.bfloat16).astype(jnp.float32)
        vcopy(n).wait()
        for m in range(step):
            t = n * step + m
            mine = slice(m * n_heads, (m + 1) * n_heads)
            mixed = jnp.dot(weights[mine], vbuf[t], preferred_element_type=jnp.float32)
            mixed = mixed + own_weight[mine] * own_values[t : t + 1, :]
            heads[pl.ds(t, n_heads, stride=tokens), :] = mixed
    columns = []
    for c in range(n_heads // per):
        column = None
        for p in range(per):
            h = c * per + p
            x = shifted(heads[h * tokens : (h + 1) * tokens, :], h // grouped, p)
            column = x if column is None else jnp.where(lane // HD == p, x, column)
        columns.append(column.astype(jnp.bfloat16))
    stacked = jnp.concatenate(columns, axis=1)
    stacked_ref[...] = stacked
    for k in reversed(range(early, parts)):
        wcopy(k).wait()
        piece = lax.dot_general(
            stacked, wobuf[k - early], (((1,), (1,)), ((), ())),
            preferred_element_type=jnp.float32,
        )
        outs[k - early][...] = piece.astype(outs[k - early].dtype)
    for k in reversed(range(early)):
        wcopy(k).wait()


def project_kernel(stacked_ref, later_ref, *outs):
    for k in reversed(range(len(outs))):
        piece = lax.dot_general(
            stacked_ref[...], later_ref[k], (((1,), (1,)), ((), ())),
            preferred_element_type=jnp.float32,
        )
        outs[k][...] = piece.astype(outs[k].dtype)


def attend_project(
    share, q_new, k_new, v_new, k_cache, v_cache, cache_len, cycle_start, out_proj, parts
):
    tokens, window, lanes = k_cache.shape
    n_heads = q_new.shape[1] // HD
    quarter = out_proj.shape[0] // parts
    chunks = 4
    smem = pl.BlockSpec(memory_space=pltpu.SMEM)
    vmem = pl.BlockSpec(memory_space=pltpu.VMEM)
    hbm = pl.BlockSpec(memory_space=pltpu.HBM)
    inputs = [
        pltpu.with_memory_space_constraint(x, pltpu.HBM)
        for x in (
            cache_len, cycle_start, q_new, k_new, v_new, k_cache, v_cache, out_proj
        )
    ]
    early = parts // 2
    piece = jax.ShapeDtypeStruct((tokens, quarter), jnp.bfloat16)
    made = pl.pallas_call(
        functools.partial(
            attend_kernel, grouped=HEADS // KV_HEADS, chunks=chunks, parts=parts
        ),
        in_specs=[smem] + [hbm] * 8,
        out_specs=[vmem] * (early + 2),
        out_shape=[piece] * early
        + [
            jax.ShapeDtypeStruct(q_new.shape, jnp.bfloat16),
            jax.ShapeDtypeStruct((parts - early, quarter, q_new.shape[1]), out_proj.dtype),
        ],
        scratch_shapes=[
            pltpu.SMEM(cache_len.shape, jnp.int32),
            pltpu.SMEM(cycle_start.shape, jnp.int32),
            pltpu.VMEM(q_new.shape, q_new.dtype),
            pltpu.VMEM(k_new.shape, k_new.dtype),
            pltpu.VMEM(v_new.shape, v_new.dtype),
            pltpu.VMEM(k_cache.shape, k_cache.dtype),
            pltpu.VMEM(v_cache.shape, v_cache.dtype),
            pltpu.VMEM((parts - early, quarter, q_new.shape[1]), out_proj.dtype),
            pltpu.VMEM((n_heads * tokens, lanes), jnp.float32),
            pltpu.VMEM((n_heads * tokens, lanes), jnp.float32),
            pltpu.VMEM((n_heads * tokens, window), jnp.float32),
            pltpu.VMEM((n_heads * tokens, lanes), jnp.float32),
            pltpu.SemaphoreType.DMA((5,)),
            pltpu.SemaphoreType.DMA((chunks,)),
            pltpu.SemaphoreType.DMA((chunks,)),
            pltpu.SemaphoreType.DMA((parts,)),
        ],
        compiler_params=pltpu.CompilerParams(vmem_limit_bytes=16 << 20),
        name="attend_project",
    )(share, *inputs)
    first, (stacked, later) = made[:early], made[early:]
    later_call = pl.pallas_call(
        project_kernel,
        in_specs=[vmem, vmem],
        out_specs=[vmem] * early,
        out_shape=[jax.ShapeDtypeStruct((tokens, quarter), jnp.float32)] + [piece] * (early - 1),
        compiler_params=pltpu.CompilerParams(vmem_limit_bytes=8 << 20),
        name="project",
    )
    rest = later_call(stacked, later)
    return list(rest) + list(first)


def expert_kernel(
    place_ref, own_ref, other_ref, gate_ref, up_ref, down_ref, keep_ref, send_ref, pieces,
    *, quarter, topk,
):
    n_role, _, _ = own_ref.shape
    n_tp = 2
    parts = n_role * n_tp
    share = place_ref[0]
    tail_at = quarter // 128 * 128
    first = quarter - tail_at
    tail = 0.0
    columns = []
    for p in range(parts):
        slot = share ^ p
        i, l = slot // n_tp, slot % n_tp
        x = jnp.where(l == 0, own_ref[i], other_ref[i])
        tail = tail + x[:, tail_at:].astype(jnp.float32)
        columns.append(x[:, :quarter])
    inputs = jnp.concatenate(columns, axis=1)
    turned = (((1,), (1,)), ((), ()))
    gate_lin = lax.dot_general(inputs, gate_ref[0], turned, preferred_element_type=jnp.float32)
    up_lin = lax.dot_general(inputs, up_ref[0], turned, preferred_element_type=jnp.float32)
    ids = own_ref[0, :, tail_at:].astype(jnp.float32)
    n_stat = 1 + topk

    def total(c):
        at = first + topk + c
        return sum(tail[:, at + p * n_stat : at + p * n_stat + 1] for p in range(3))

    scale = lax.rsqrt(total(0) / (parts * quarter) + epsilon)
    picked = [total(1 + k) * scale for k in range(topk)]
    top = functools.reduce(jnp.maximum, picked)
    lifted = [jnp.exp(x - top) for x in picked]
    expert = place_ref[1].astype(jnp.float32)
    mine = sum(
        jnp.where(ids[:, first + k : first + k + 1] == expert, lifted[k], 0.0)
        for k in range(topk)
    )
    weight = mine / sum(lifted)
    gate_lin = gate_lin * scale
    up_lin = up_lin * scale
    activated = gate_lin * jax.nn.sigmoid(1.702 * gate_lin) * (up_lin + 1.0)
    result = jnp.dot(
        activated.astype(jnp.bfloat16), down_ref[0], preferred_element_type=jnp.float32
    )
    result = result * weight
    for p in range(parts):
        pieces[p ^ share] = result[:, p * quarter : (p + 1) * quarter].astype(jnp.bfloat16)
    for i in range(n_role):
        keep_ref[i] = pieces[i * n_tp]
        send_ref[i] = pieces[i * n_tp + 1]


def run_expert(place, own, other, w_gate, w_up, w_down, quarter, topk):
    n_role, items, _ = own.shape
    smem = pl.BlockSpec(memory_space=pltpu.SMEM)
    vmem = pl.BlockSpec(memory_space=pltpu.VMEM)
    shape = jax.ShapeDtypeStruct((n_role, items, quarter), jnp.bfloat16)
    return pl.pallas_call(
        functools.partial(expert_kernel, quarter=quarter, topk=topk),
        in_specs=[smem] + [vmem] * 5,
        out_specs=[vmem, vmem],
        out_shape=[shape, shape],
        scratch_shapes=[pltpu.VMEM((2 * n_role, items, quarter), jnp.bfloat16)],
        compiler_params=pltpu.CompilerParams(vmem_limit_bytes=24 << 20),
        name="expert",
    )(place, own, other, w_gate, w_up, w_down)


def three_parts(x):
    high = x.astype(jnp.bfloat16).astype(jnp.float32)
    rest = x - high
    middle = rest.astype(jnp.bfloat16).astype(jnp.float32)
    return high, middle, rest - middle


def pack_kernel(own_ref, *rest, moved):
    arrived, rest = rest[:moved], rest[moved:]
    residual_ref, gain_ref, router_ref, ids_ref, attended_ref, packed_ref = rest
    stream = residual_ref[...].astype(jnp.float32) + own_ref[...]
    for ref in arrived:
        stream = stream + ref[...].astype(jnp.float32)
    attended_ref[...] = stream.astype(jnp.bfloat16)
    tokens, quarter = stream.shape
    topk = ids_ref.shape[0]
    scaled = (stream * gain_ref[...]).astype(jnp.bfloat16)
    squares = jnp.sum(stream * stream, axis=1, keepdims=True)
    logits = lax.dot_general(
        scaled, router_ref[...], (((1,), (1,)), ((), ())), preferred_element_type=jnp.float32
    )
    names = lax.broadcasted_iota(jnp.int32, logits.shape, 1).astype(jnp.float32)
    eye = (
        lax.broadcasted_iota(jnp.int32, (topk, topk), 0)
        == lax.broadcasted_iota(jnp.int32, (topk, topk), 1)
    )
    ids = lax.dot_general(
        ids_ref[...].astype(jnp.float32).astype(jnp.bfloat16), eye.astype(jnp.bfloat16),
        (((0,), (0,)), ((), ())), preferred_element_type=jnp.float32,
    )
    stats = [squares]
    columns = []
    for k in range(topk):
        chosen = ids[:, k : k + 1]
        columns.append(chosen)
        stats.append(jnp.sum(jnp.where(names == chosen, logits, 0.0), axis=1, keepdims=True))
    split = [three_parts(x) for x in stats]
    for p in range(3):
        columns.extend(x[p] for x in split)
    tail_at = quarter // 128 * 128
    first = quarter - tail_at
    packed_ref[:, :quarter] = scaled
    tile = packed_ref[:, tail_at : tail_at + 128]
    lane = lax.broadcasted_iota(jnp.int32, (tokens, 128), 1)
    tail = jnp.zeros((tokens, 128), jnp.float32)
    for c, x in enumerate(columns):
        tail = jnp.where(lane == first + c, x, tail)
    packed_ref[:, tail_at : tail_at + 128] = jnp.where(
        lane < first, tile.astype(jnp.float32), tail
    ).astype(jnp.bfloat16)


def run_pack(own, arrived, residual, gain, router, route_ids):
    tokens, quarter = residual.shape
    vmem = pl.BlockSpec(memory_space=pltpu.VMEM)
    lanes = quarter // 128 * 128 + 128
    assert quarter % 128 + 4 * route_ids.shape[0] + 3 <= 128
    return pl.pallas_call(
        functools.partial(pack_kernel, moved=len(arrived)),
        in_specs=[vmem] * (5 + len(arrived)),
        out_specs=[vmem, vmem],
        out_shape=[
            jax.ShapeDtypeStruct((tokens, quarter), jnp.bfloat16),
            jax.ShapeDtypeStruct((tokens, lanes), jnp.bfloat16),
        ],
        compiler_params=pltpu.CompilerParams(vmem_limit_bytes=4 << 20),
        cost_estimate=pl.CostEstimate(flops=COVER, transcendentals=0, bytes_accessed=1 << 20),
        name="pack",
    )(own, *arrived, residual, gain, router, route_ids)


def select_kernel(expert_ref, *rest, n_far, n_near, cap, topk, quarter):
    blocks, rest = rest[:n_far], rest[n_far:]
    rows, picks = rest[:n_near], rest[n_near:]
    tokens, _ = blocks[0].shape
    tail_at = quarter // 128 * 128
    first = quarter - tail_at
    stacked = jnp.concatenate([ref[...] for ref in blocks], axis=0)
    ids = stacked[:, tail_at:].astype(jnp.float32).T
    n_all = n_far * tokens
    source = lax.broadcasted_iota(jnp.int32, (n_all, n_all), 0)
    target = lax.broadcasted_iota(jnp.int32, (n_all, n_all), 1)
    same = source // tokens == target // tokens
    before = jnp.where(same & (source < target), 1.0, 0.0).astype(jnp.bfloat16)
    slot = lax.broadcasted_iota(jnp.int32, (n_far * cap, n_all), 0).astype(jnp.float32)
    base = lax.broadcasted_iota(jnp.int32, (1, n_all), 1) // tokens * cap
    hits = []
    for j in range(n_near):
        expert = expert_ref[j].astype(jnp.float32)
        hit = jnp.zeros((1, n_all), jnp.float32)
        for k in range(topk):
            hit = hit + jnp.where(ids[first + k : first + k + 1, :] == expert, 1.0, 0.0)
        hits.append(hit)
    line = lax.broadcasted_iota(jnp.int32, (8, n_all), 0)
    table = jnp.zeros((8, n_all), jnp.float32)
    for j in range(n_near):
        table = jnp.where(line == j, hits[j], table)
    ranks = jnp.dot(table.astype(jnp.bfloat16), before, preferred_element_type=jnp.float32)
    for j in reversed(range(n_near)):
        at = jnp.where(hits[j] > 0.0, ranks[j : j + 1, :] + base.astype(jnp.float32), -1.0)
        pick = jnp.where(at == slot, 1.0, 0.0).astype(jnp.bfloat16)
        picks[j][...] = pick
        rows[j][...] = jnp.dot(pick, stacked, preferred_element_type=jnp.float32).astype(
            jnp.bfloat16
        )


def run_select(experts, blocks, n_near, cap, topk, quarter):
    tokens, lanes = blocks[0].shape
    n_far = len(blocks)
    vmem = pl.BlockSpec(memory_space=pltpu.VMEM)
    outs = [jax.ShapeDtypeStruct((n_far * cap, lanes), jnp.bfloat16)] * n_near
    outs += [jax.ShapeDtypeStruct((n_far * cap, n_far * tokens), jnp.bfloat16)] * n_near
    made = pl.pallas_call(
        functools.partial(
            select_kernel, n_far=n_far, n_near=n_near, cap=cap, topk=topk, quarter=quarter
        ),
        in_specs=[pl.BlockSpec(memory_space=pltpu.SMEM)] + [vmem] * n_far,
        out_specs=[vmem] * len(outs),
        out_shape=outs,
        compiler_params=pltpu.CompilerParams(vmem_limit_bytes=12 << 20),
        name="select",
    )(experts, *blocks)
    return made[:n_near], made[n_near:]


def spread_kernel(*refs, n_near, n_role, n_far):
    rows, refs = refs[: n_near * n_role], refs[n_near * n_role :]
    picks, outs = refs[:n_near], refs[n_near:]
    total = 0.0
    for j in range(n_near):
        row = 0.0
        for i in range(n_role):
            row = row + rows[j * n_role + i][...].astype(jnp.float32)
        total = total + lax.dot_general(
            picks[j][...], row.astype(jnp.bfloat16), (((0,), (0,)), ((), ())),
            preferred_element_type=jnp.float32,
        )
    tokens = total.shape[0] // n_far
    for n in range(n_far):
        outs[n][...] = total[n * tokens : (n + 1) * tokens].astype(outs[n].dtype)


def run_spread(rows, picks, n_role, n_far):
    n_near = len(picks)
    tokens = picks[0].shape[1] // n_far
    vmem = pl.BlockSpec(memory_space=pltpu.VMEM)
    quarter = rows[0].shape[1]
    kinds = [jnp.float32] + [jnp.bfloat16] * (n_far - 1)
    return pl.pallas_call(
        functools.partial(spread_kernel, n_near=n_near, n_role=n_role, n_far=n_far),
        in_specs=[vmem] * (len(rows) + n_near),
        out_specs=[vmem] * n_far,
        out_shape=[jax.ShapeDtypeStruct((tokens, quarter), kind) for kind in kinds],
        compiler_params=pltpu.CompilerParams(vmem_limit_bytes=12 << 20),
        name="spread",
    )(*rows, *picks)


def swap_table(mesh, grp_of, role_flip, tp_flip):
    names = mesh.axis_names
    sizes = [mesh.shape[n] for n in names]
    pairs = []
    for flat in range(math.prod(sizes)):
        at = dict(zip(names, [int(v) for v in np.unravel_index(flat, sizes)]))
        to = dict(
            role=at["role"] ^ role_flip, tp=at["tp"] ^ tp_flip, grp=grp_of(at["grp"])
        )
        pairs.append((flat, int(np.ravel_multi_index([to[n] for n in names], sizes))))
    return pairs


def make_local(mesh):
    n_role, n_grp, n_tp = (mesh.shape[n] for n in ("role", "grp", "tp"))
    n_near = 2 if n_grp % 2 == 0 else 1
    n_far = n_grp // n_near
    xor_far = n_far & (n_far - 1) == 0
    names = mesh.axis_names

    def send(x, near=0, role=0, tp=0):
        return lax.ppermute(x, names, swap_table(mesh, lambda g: g ^ near, role, tp))

    def send_far(x, k):
        def grp_of(g):
            far, near = divmod(g, n_near)
            return (far ^ k if xor_far else (far + k) % n_far) * n_near + near

        return lax.ppermute(x, names, swap_table(mesh, grp_of, 0, 0))

    def local(
        q_new, k_new, v_new, k_cache, v_cache, cache_len, cycle_start, residual,
        out_proj, norm_gain, router, route_ids, w_gate, w_up, w_down,
    ):
        role, grp, tp = (lax.axis_index(n) for n in ("role", "grp", "tp"))
        tokens, quarter = residual.shape
        topk = route_ids.shape[1]
        experts = n_grp * w_gate.shape[0]
        cap = max(3, tokens * topk // experts + 2)
        far, near = grp // n_near, grp % n_near
        share = role * n_tp + tp
        parts = n_role * n_tp
        place = share.astype(jnp.int32).reshape(1)
        pieces = attend_project(
            place, q_new, k_new, v_new, k_cache, v_cache, cache_len, cycle_start, out_proj.T, parts
        )
        moved = []
        for k in range(1, parts):
            moved.append(send(pieces[k], role=k // n_tp, tp=k % n_tp))
        gain = lax.dynamic_slice_in_dim(norm_gain, share * quarter, quarter, 0).reshape(1, quarter)
        attended, packed = run_pack(pieces[0], moved, residual, gain, router.T, route_ids.T)
        blocks = [packed] + [send_far(packed, k) for k in range(1, n_far)]
        experts_near = jnp.stack([far * n_near + (near ^ j) for j in range(n_near)])
        rows, picks = run_select(
            experts_near.astype(jnp.int32), blocks, n_near, cap, topk, quarter
        )
        arrived = {(0, 0): rows[0]}
        for j in range(n_near):
            for i in range(n_role):
                if (j, i) != (0, 0):
                    arrived[j, i] = send(rows[j], near=j, role=i)
        half = jnp.stack(
            [jnp.concatenate([arrived[j, i] for j in range(n_near)], 0) for i in range(n_role)]
        )
        other = send(half, tp=1)
        place = jnp.stack([share, grp]).astype(jnp.int32)
        kept, sent = run_expert(
            place, half, other, jnp.swapaxes(w_gate, 1, 2), jnp.swapaxes(w_up, 1, 2), w_down,
            quarter, topk,
        )
        acc = kept.astype(jnp.float32) + send(sent, tp=1).astype(jnp.float32)
        acc = acc.astype(jnp.bfloat16).reshape(n_role, n_near, n_far * cap, quarter)
        back = []
        for j in range(n_near):
            for i in range(n_role):
                piece = acc[i, j]
                if (j, i) != (0, 0):
                    piece = send(piece, near=j, role=i)
                back.append(piece)
        spread = run_spread(back, picks, n_role, n_far)
        mix = spread[0].astype(jnp.float32)
        for k in range(1, n_far):
            mix = mix + send_far(spread[k], k if xor_far else n_far - k).astype(jnp.float32)
        return (attended, mix.astype(jnp.bfloat16))

    return local


def solution(mesh):
    placed = (
        P("grp", ("role", "tp")),
        P("grp", ("role", "tp")),
        P("grp", ("role", "tp")),
        P("grp", None, ("role", "tp")),
        P("grp", None, ("role", "tp")),
        P("grp"),
        P("grp"),
        P("grp", ("role", "tp")),
        P(("role", "tp"), None),
        P(),
        P(("role", "tp"), None),
        P("grp", None),
        P("grp", None, ("role", "tp")),
        P("grp", None, ("role", "tp")),
        P("grp", ("role", "tp"), None),
    )
    local = make_local(mesh)

    return jax.shard_map(
        local,
        mesh=mesh,
        in_specs=placed,
        out_specs=(P("grp", ("role", "tp")), P("grp", ("role", "tp"))),
        check_vma=False,
    )
```

```python
import functools
import math

import jax
import jax.numpy as jnp
import numpy as np
from jax import lax
from jax.experimental import pallas as pl
from jax.experimental.pallas import tpu as pltpu
from jax.sharding import PartitionSpec as P


HEADS = 64
KV_HEADS = 8
HD = 64


epsilon = 1e-05
COVER = 1 << 33


def attend_kernel(
    share_ref, len_hbm, start_hbm, q_hbm, kn_hbm, vn_hbm, k_hbm, v_hbm, wo_hbm,
    *rest, grouped, chunks, parts,
):
    early = parts // 2
    outs, (stacked_ref, later_ref), rest = rest[:early], rest[early : early + 2], rest[early + 2 :]
    len_ref, start_ref, q_ref, kn_ref, vn_ref, kbuf, vbuf, wobuf = rest[:8]
    queries, heads, scores, products, small, ksem, vsem, wsem = rest[8:]
    tokens, window, lanes = k_hbm.shape
    pairs = (
        (q_hbm, q_ref), (kn_hbm, kn_ref), (vn_hbm, vn_ref), (len_hbm, len_ref),
        (start_hbm, start_ref),
    )
    firsts = [pltpu.make_async_copy(a, b, small.at[n]) for n, (a, b) in enumerate(pairs)]
    for copy in firsts:
        copy.start()
    n_heads = q_ref.shape[1] // HD
    step = tokens // chunks
    rows = wo_hbm.shape[0] // parts

    def kcopy(n):
        at = pl.ds(n * step, step)
        return pltpu.make_async_copy(k_hbm.at[at], kbuf.at[at], ksem.at[n])

    def vcopy(n):
        at = pl.ds(n * step, step)
        return pltpu.make_async_copy(v_hbm.at[at], vbuf.at[at], vsem.at[n])

    def wrows(k):
        return pl.ds(pl.multiple_of((share_ref[0] ^ k) * rows, 16), rows)

    def wcopy(k):
        target = wobuf.at[k - early] if k >= early else later_ref.at[k]
        return pltpu.make_async_copy(wo_hbm.at[wrows(k)], target, wsem.at[k])

    for n in range(chunks):
        kcopy(n).start()
        vcopy(n).start()
    for copy in firsts:
        copy.wait()
    lane = lax.broadcasted_iota(jnp.int32, (tokens, lanes), 1)
    per = lanes // HD

    def shifted(x, source, target):
        if source == target:
            return x
        return pltpu.roll(x, ((target - source) * HD) % lanes, 1)

    for h in range(n_heads):
        at = h // per * lanes
        x = q_ref[:, at : at + lanes].astype(jnp.float32)
        kv = h // grouped
        x = jnp.where(lane // HD == kv, shifted(x, h % per, kv), 0.0)
        queries[h * tokens : (h + 1) * tokens, :] = x
    factor = HD ** (-0.5)
    slots = lax.broadcasted_iota(jnp.int32, (1, window), 1)
    own_keys = kn_ref[...].astype(jnp.float32)
    own_values = vn_ref[...].astype(jnp.float32)
    block = step * n_heads
    for n in range(chunks):
        kcopy(n).wait()
        if n == 0:
            for k in reversed(range(parts)):
                wcopy(k).start()
        for t in range(n * step, (n + 1) * step):
            query = queries[pl.ds(t, n_heads, stride=tokens), :]
            dots = lax.dot_general(
                query.astype(jnp.bfloat16), kbuf[t], (((1,), (1,)), ((), ())),
                preferred_element_type=jnp.float32,
            )
            age = slots - start_ref[t]
            age = jnp.where(age < 0, age + window, age)
            at = pl.ds(t * n_heads, n_heads)
            scores[at, :] = jnp.where(age < len_ref[t], factor * dots, -1e30)
            products[at, :] = query * own_keys[t : t + 1, :]
    for n in range(chunks):
        at = pl.ds(n * block, block)
        masked = scores[at, :]
        own = factor * jnp.sum(products[at, :], axis=1, keepdims=True)
        highest = jnp.maximum(jnp.max(masked, axis=1, keepdims=True), own)
        lifted = jnp.exp(masked - highest)
        own_lift = jnp.exp(own - highest)
        denominator = jnp.sum(lifted, axis=1, keepdims=True) + own_lift
        weights = (lifted / denominator).astype(jnp.bfloat16)
        own_weight = (own_lift / denominator).astype(jnp.bfloat16).astype(jnp.float32)
        vcopy(n).wait()
        for m in range(step):
            t = n * step + m
            mine = slice(m * n_heads, (m + 1) * n_heads)
            mixed = jnp.dot(weights[mine], vbuf[t], preferred_element_type=jnp.float32)
            mixed = mixed + own_weight[mine] * own_values[t : t + 1, :]
            heads[pl.ds(t, n_heads, stride=tokens), :] = mixed
    columns = []
    for c in range(n_heads // per):
        column = None
        for p in range(per):
            h = c * per + p
            x = shifted(heads[h * tokens : (h + 1) * tokens, :], h // grouped, p)
            column = x if column is None else jnp.where(lane // HD == p, x, column)
        columns.append(column.astype(jnp.bfloat16))
    stacked = jnp.concatenate(columns, axis=1)
    stacked_ref[...] = stacked
    for k in reversed(range(early, parts)):
        wcopy(k).wait()
        piece = lax.dot_general(
            stacked, wobuf[k - early], (((1,), (1,)), ((), ())),
            preferred_element_type=jnp.float32,
        )
        outs[k - early][...] = piece.astype(outs[k - early].dtype)
    for k in reversed(range(early)):
        wcopy(k).wait()


def project_kernel(stacked_ref, later_ref, *outs):
    for k in reversed(range(len(outs))):
        piece = lax.dot_general(
            stacked_ref[...], later_ref[k], (((1,), (1,)), ((), ())),
            preferred_element_type=jnp.float32,
        )
        outs[k][...] = piece.astype(outs[k].dtype)


def attend_project(
    share, q_new, k_new, v_new, k_cache, v_cache, cache_len, cycle_start, out_proj, parts
):
    tokens, window, lanes = k_cache.shape
    n_heads = q_new.shape[1] // HD
    quarter = out_proj.shape[0] // parts
    chunks = 4
    smem = pl.BlockSpec(memory_space=pltpu.SMEM)
    vmem = pl.BlockSpec(memory_space=pltpu.VMEM)
    hbm = pl.BlockSpec(memory_space=pltpu.HBM)
    inputs = [
        pltpu.with_memory_space_constraint(x, pltpu.HBM)
        for x in (
            cache_len, cycle_start, q_new, k_new, v_new, k_cache, v_cache, out_proj
        )
    ]
    early = parts // 2
    piece = jax.ShapeDtypeStruct((tokens, quarter), jnp.bfloat16)
    made = pl.pallas_call(
        functools.partial(
            attend_kernel, grouped=HEADS // KV_HEADS, chunks=chunks, parts=parts
        ),
        in_specs=[smem] + [hbm] * 8,
        out_specs=[vmem] * (early + 2),
        out_shape=[piece] * early
        + [
            jax.ShapeDtypeStruct(q_new.shape, jnp.bfloat16),
            jax.ShapeDtypeStruct((parts - early, quarter, q_new.shape[1]), out_proj.dtype),
        ],
        scratch_shapes=[
            pltpu.SMEM(cache_len.shape, jnp.int32),
            pltpu.SMEM(cycle_start.shape, jnp.int32),
            pltpu.VMEM(q_new.shape, q_new.dtype),
            pltpu.VMEM(k_new.shape, k_new.dtype),
            pltpu.VMEM(v_new.shape, v_new.dtype),
            pltpu.VMEM(k_cache.shape, k_cache.dtype),
            pltpu.VMEM(v_cache.shape, v_cache.dtype),
            pltpu.VMEM((parts - early, quarter, q_new.shape[1]), out_proj.dtype),
            pltpu.VMEM((n_heads * tokens, lanes), jnp.float32),
            pltpu.VMEM((n_heads * tokens, lanes), jnp.float32),
            pltpu.VMEM((n_heads * tokens, window), jnp.float32),
            pltpu.VMEM((n_heads * tokens, lanes), jnp.float32),
            pltpu.SemaphoreType.DMA((5,)),
            pltpu.SemaphoreType.DMA((chunks,)),
            pltpu.SemaphoreType.DMA((chunks,)),
            pltpu.SemaphoreType.DMA((parts,)),
        ],
        compiler_params=pltpu.CompilerParams(vmem_limit_bytes=16 << 20),
        name="attend_project",
    )(share, *inputs)
    first, (stacked, later) = made[:early], made[early:]
    later_call = pl.pallas_call(
        project_kernel,
        in_specs=[vmem, vmem],
        out_specs=[vmem] * early,
        out_shape=[jax.ShapeDtypeStruct((tokens, quarter), jnp.float32)] + [piece] * (early - 1),
        compiler_params=pltpu.CompilerParams(vmem_limit_bytes=8 << 20),
        name="project",
    )
    rest = later_call(stacked, later)
    return list(rest) + list(first)


def for_each_share(place_ref, parts, body):
    for share in range(parts):
        pl.when(place_ref[0] == share)(functools.partial(body, share))


def window_of(place, quarter):
    first, last = place * quarter, (place + 1) * quarter
    start = first // 128 * 128
    return slice(start, last), first - start


def partial_products(refs, places, gate_ref, up_ref, quarter):
    turned = (((1,), (1,)), ((), ()))
    gate_lin = up_lin = 0.0
    for x, p in zip(refs, places):
        at, shift = window_of(p, quarter)
        x = x[:, :quarter]
        if shift:
            x = jnp.concatenate([jnp.zeros((x.shape[0], shift), x.dtype), x], axis=1)
        gate_lin = gate_lin + lax.dot_general(
            x, gate_ref[0, :, at], turned, preferred_element_type=jnp.float32
        )
        up_lin = up_lin + lax.dot_general(
            x, up_ref[0, :, at], turned, preferred_element_type=jnp.float32
        )
    return gate_lin, up_lin


def down_products(activated, weight, place, down_ref, quarter):
    at, shift = window_of(place, quarter)
    result = jnp.dot(activated, down_ref[0, :, at], preferred_element_type=jnp.float32) * weight
    return result[:, shift:].astype(jnp.bfloat16)


def first_kernel(place_ref, own_ref, gate_ref, up_ref, gate_out, up_out, *, quarter, n_tp):
    n_role = own_ref.shape[0]

    def body(share):
        places = [share ^ (i * n_tp) for i in range(n_role)]
        gate_out[...], up_out[...] = partial_products(
            [own_ref[i] for i in range(n_role)], places, gate_ref, up_ref, quarter
        )

    for_each_share(place_ref, n_role * n_tp, body)


def second_kernel(
    place_ref, own_ref, other_ref, gate_in, up_in, gate_ref, up_ref, down_ref, send_ref,
    activated_ref, weight_ref, *, quarter, topk, n_tp,
):
    def body(share):
        second_body(
            share, place_ref, own_ref, other_ref, gate_in, up_in, gate_ref, up_ref, down_ref,
            send_ref, activated_ref, weight_ref, quarter, topk, n_tp,
        )

    for_each_share(place_ref, own_ref.shape[0] * n_tp, body)


def second_body(
    share, place_ref, own_ref, other_ref, gate_in, up_in, gate_ref, up_ref, down_ref,
    send_ref, activated_ref, weight_ref, quarter, topk, n_tp,
):
    n_role, _, _ = own_ref.shape
    tail_at = quarter // 128 * 128
    first = quarter - tail_at
    places = [share ^ (i * n_tp + 1) for i in range(n_role)]
    gate_lin, up_lin = partial_products(
        [other_ref[i] for i in range(n_role)], places, gate_ref, up_ref, quarter
    )
    tail = 0.0
    for ref in (own_ref, other_ref):
        for i in range(n_role):
            tail = tail + ref[i, :, tail_at:].astype(jnp.float32)
    ids = pltpu.roll(own_ref[0, :, tail_at:].astype(jnp.float32), topk + 1, 1)
    n_stat = 1 + topk
    span = tail.shape[1]
    tail = tail + pltpu.roll(tail, span - n_stat, 1) + pltpu.roll(tail, span - 2 * n_stat, 1)
    at = first + topk
    scale = lax.rsqrt(tail[:, at : at + 1] / down_ref.shape[2] + epsilon)
    lane = lax.broadcasted_iota(jnp.int32, tail.shape, 1)
    chosen = (lane > at) & (lane <= at + topk)
    picked = jnp.where(chosen, tail * scale, -1e30)
    lifted = jnp.exp(picked - jnp.max(picked, axis=1, keepdims=True))
    expert = place_ref[1].astype(jnp.float32)
    mine = jnp.where(chosen & (ids == expert), lifted, 0.0)
    weight = jnp.sum(mine, axis=1, keepdims=True) / jnp.sum(lifted, axis=1, keepdims=True)
    gate_lin = (gate_lin + gate_in[...]) * scale
    up_lin = (up_lin + up_in[...]) * scale
    activated = gate_lin * jax.nn.sigmoid(1.702 * gate_lin) * (up_lin + 1.0)
    activated = activated.astype(jnp.bfloat16)
    activated_ref[...] = activated
    weight_ref[...] = jnp.broadcast_to(weight, weight_ref.shape)
    for i in range(n_role):
        send_ref[i] = down_products(activated, weight, places[i], down_ref, quarter)


def third_kernel(place_ref, activated_ref, weight_ref, down_ref, keep_ref, *, quarter, n_tp):
    n_role = keep_ref.shape[0]

    def body(share):
        weight = weight_ref[:, :1]
        for i in range(n_role):
            place = share ^ (i * n_tp)
            keep_ref[i] = down_products(activated_ref[...], weight, place, down_ref, quarter)

    for_each_share(place_ref, n_role * n_tp, body)


def run_first(place, own, w_gate, w_up, quarter, n_tp):
    vmem = pl.BlockSpec(memory_space=pltpu.VMEM)
    partial = jax.ShapeDtypeStruct((own.shape[1], w_gate.shape[1]), jnp.float32)
    return pl.pallas_call(
        functools.partial(first_kernel, quarter=quarter, n_tp=n_tp),
        in_specs=[pl.BlockSpec(memory_space=pltpu.SMEM)] + [vmem] * 3,
        out_specs=[vmem, vmem],
        out_shape=[partial, partial],
        compiler_params=pltpu.CompilerParams(vmem_limit_bytes=16 << 20),
        name="expert_first",
    )(place, own, w_gate, w_up)


def run_second(place, own, other, partials, w_gate, w_up, w_down, quarter, topk, n_tp):
    n_role, items, _ = own.shape
    vmem = pl.BlockSpec(memory_space=pltpu.VMEM)
    return pl.pallas_call(
        functools.partial(second_kernel, quarter=quarter, topk=topk, n_tp=n_tp),
        in_specs=[pl.BlockSpec(memory_space=pltpu.SMEM)] + [vmem] * 7,
        out_specs=[vmem] * 3,
        out_shape=[
            jax.ShapeDtypeStruct((n_role, items, quarter), jnp.bfloat16),
            jax.ShapeDtypeStruct((items, w_gate.shape[1]), jnp.bfloat16),
            jax.ShapeDtypeStruct((items, 128), jnp.float32),
        ],
        compiler_params=pltpu.CompilerParams(vmem_limit_bytes=24 << 20),
        name="expert_second",
    )(place, own, other, *partials, w_gate, w_up, w_down)


def run_third(place, activated, weight, w_down, n_role, quarter, n_tp):
    vmem = pl.BlockSpec(memory_space=pltpu.VMEM)
    items = activated.shape[0]
    return pl.pallas_call(
        functools.partial(third_kernel, quarter=quarter, n_tp=n_tp),
        in_specs=[pl.BlockSpec(memory_space=pltpu.SMEM)] + [vmem] * 3,
        out_specs=vmem,
        out_shape=jax.ShapeDtypeStruct((n_role, items, quarter), jnp.bfloat16),
        compiler_params=pltpu.CompilerParams(vmem_limit_bytes=12 << 20),
        name="expert_third",
    )(place, activated, weight, w_down)


def three_parts(x):
    high = x.astype(jnp.bfloat16).astype(jnp.float32)
    rest = x - high
    middle = rest.astype(jnp.bfloat16).astype(jnp.float32)
    return high, middle, rest - middle


def pack_kernel(own_ref, *rest, moved):
    arrived, rest = rest[:moved], rest[moved:]
    residual_ref, gain_ref, router_ref, ids_ref, attended_ref, packed_ref = rest
    stream = residual_ref[...].astype(jnp.float32) + own_ref[...]
    for ref in arrived:
        stream = stream + ref[...].astype(jnp.float32)
    attended_ref[...] = stream.astype(jnp.bfloat16)
    tokens, quarter = stream.shape
    topk = ids_ref.shape[0]
    scaled = (stream * gain_ref[...]).astype(jnp.bfloat16)
    squares = jnp.sum(stream * stream, axis=1, keepdims=True)
    logits = lax.dot_general(
        scaled, router_ref[...], (((1,), (1,)), ((), ())), preferred_element_type=jnp.float32
    )
    names = lax.broadcasted_iota(jnp.int32, logits.shape, 1).astype(jnp.float32)
    eye = (
        lax.broadcasted_iota(jnp.int32, (topk, topk), 0)
        == lax.broadcasted_iota(jnp.int32, (topk, topk), 1)
    )
    ids = lax.dot_general(
        ids_ref[...].astype(jnp.float32).astype(jnp.bfloat16), eye.astype(jnp.bfloat16),
        (((0,), (0,)), ((), ())), preferred_element_type=jnp.float32,
    )
    stats = [squares]
    columns = []
    for k in range(topk):
        chosen = ids[:, k : k + 1]
        columns.append(chosen)
        stats.append(jnp.sum(jnp.where(names == chosen, logits, 0.0), axis=1, keepdims=True))
    split = [three_parts(x) for x in stats]
    for p in range(3):
        columns.extend(x[p] for x in split)
    tail_at = quarter // 128 * 128
    first = quarter - tail_at
    packed_ref[:, :quarter] = scaled
    tile = packed_ref[:, tail_at : tail_at + 128]
    lane = lax.broadcasted_iota(jnp.int32, (tokens, 128), 1)
    tail = jnp.zeros((tokens, 128), jnp.float32)
    for c, x in enumerate(columns):
        tail = jnp.where(lane == first + c, x, tail)
    packed_ref[:, tail_at : tail_at + 128] = jnp.where(
        lane < first, tile.astype(jnp.float32), tail
    ).astype(jnp.bfloat16)


def run_pack(own, arrived, residual, gain, router, route_ids):
    tokens, quarter = residual.shape
    vmem = pl.BlockSpec(memory_space=pltpu.VMEM)
    lanes = quarter // 128 * 128 + 128
    assert quarter % 128 + 4 * route_ids.shape[0] + 3 <= 128
    return pl.pallas_call(
        functools.partial(pack_kernel, moved=len(arrived)),
        in_specs=[vmem] * (5 + len(arrived)),
        out_specs=[vmem, vmem],
        out_shape=[
            jax.ShapeDtypeStruct((tokens, quarter), jnp.bfloat16),
            jax.ShapeDtypeStruct((tokens, lanes), jnp.bfloat16),
        ],
        compiler_params=pltpu.CompilerParams(vmem_limit_bytes=4 << 20),
        cost_estimate=pl.CostEstimate(flops=COVER, transcendentals=0, bytes_accessed=1 << 20),
        name="pack",
    )(own, *arrived, residual, gain, router, route_ids)


def select_kernel(expert_ref, *rest, n_far, n_near, cap, topk, quarter):
    blocks, rest = rest[:n_far], rest[n_far:]
    rows, picks = rest[:n_near], rest[n_near:]
    tokens, _ = blocks[0].shape
    tail_at = quarter // 128 * 128
    first = quarter - tail_at
    stacked = jnp.concatenate([ref[...] for ref in blocks], axis=0)
    ids = stacked[:, tail_at:].astype(jnp.float32).T
    n_all = n_far * tokens
    source = lax.broadcasted_iota(jnp.int32, (n_all, n_all), 0)
    target = lax.broadcasted_iota(jnp.int32, (n_all, n_all), 1)
    same = source // tokens == target // tokens
    before = jnp.where(same & (source < target), 1.0, 0.0).astype(jnp.bfloat16)
    slot = lax.broadcasted_iota(jnp.int32, (n_far * cap, n_all), 0).astype(jnp.float32)
    base = lax.broadcasted_iota(jnp.int32, (1, n_all), 1) // tokens * cap
    hits = []
    for j in range(n_near):
        expert = expert_ref[j].astype(jnp.float32)
        hit = jnp.zeros((1, n_all), jnp.float32)
        for k in range(topk):
            hit = hit + jnp.where(ids[first + k : first + k + 1, :] == expert, 1.0, 0.0)
        hits.append(hit)
    line = lax.broadcasted_iota(jnp.int32, (8, n_all), 0)
    table = jnp.zeros((8, n_all), jnp.float32)
    for j in range(n_near):
        table = jnp.where(line == j, hits[j], table)
    ranks = jnp.dot(table.astype(jnp.bfloat16), before, preferred_element_type=jnp.float32)
    for j in reversed(range(n_near)):
        at = jnp.where(hits[j] > 0.0, ranks[j : j + 1, :] + base.astype(jnp.float32), -1.0)
        pick = jnp.where(at == slot, 1.0, 0.0).astype(jnp.bfloat16)
        picks[j][...] = pick
        rows[j][...] = jnp.dot(pick, stacked, preferred_element_type=jnp.float32).astype(
            jnp.bfloat16
        )


def run_select(experts, blocks, n_near, cap, topk, quarter):
    tokens, lanes = blocks[0].shape
    n_far = len(blocks)
    vmem = pl.BlockSpec(memory_space=pltpu.VMEM)
    outs = [jax.ShapeDtypeStruct((n_far * cap, lanes), jnp.bfloat16)] * n_near
    outs += [jax.ShapeDtypeStruct((n_far * cap, n_far * tokens), jnp.bfloat16)] * n_near
    made = pl.pallas_call(
        functools.partial(
            select_kernel, n_far=n_far, n_near=n_near, cap=cap, topk=topk, quarter=quarter
        ),
        in_specs=[pl.BlockSpec(memory_space=pltpu.SMEM)] + [vmem] * n_far,
        out_specs=[vmem] * len(outs),
        out_shape=outs,
        compiler_params=pltpu.CompilerParams(vmem_limit_bytes=12 << 20),
        name="select",
    )(experts, *blocks)
    return made[:n_near], made[n_near:]


def spread_kernel(*refs, n_near, n_role, n_far):
    rows, refs = refs[: n_near * n_role], refs[n_near * n_role :]
    picks, outs = refs[:n_near], refs[n_near:]
    total = 0.0
    for j in range(n_near):
        row = 0.0
        for i in range(n_role):
            row = row + rows[j * n_role + i][...].astype(jnp.float32)
        total = total + lax.dot_general(
            picks[j][...], row.astype(jnp.bfloat16), (((0,), (0,)), ((), ())),
            preferred_element_type=jnp.float32,
        )
    tokens = total.shape[0] // n_far
    for n in range(n_far):
        outs[n][...] = total[n * tokens : (n + 1) * tokens].astype(outs[n].dtype)


def run_spread(rows, picks, n_role, n_far):
    n_near = len(picks)
    tokens = picks[0].shape[1] // n_far
    vmem = pl.BlockSpec(memory_space=pltpu.VMEM)
    quarter = rows[0].shape[1]
    kinds = [jnp.float32] + [jnp.bfloat16] * (n_far - 1)
    return pl.pallas_call(
        functools.partial(spread_kernel, n_near=n_near, n_role=n_role, n_far=n_far),
        in_specs=[vmem] * (len(rows) + n_near),
        out_specs=[vmem] * n_far,
        out_shape=[jax.ShapeDtypeStruct((tokens, quarter), kind) for kind in kinds],
        compiler_params=pltpu.CompilerParams(vmem_limit_bytes=12 << 20),
        name="spread",
    )(*rows, *picks)


def swap_table(mesh, grp_of, role_flip, tp_flip):
    names = mesh.axis_names
    sizes = [mesh.shape[n] for n in names]
    pairs = []
    for flat in range(math.prod(sizes)):
        at = dict(zip(names, [int(v) for v in np.unravel_index(flat, sizes)]))
        to = dict(
            role=at["role"] ^ role_flip, tp=at["tp"] ^ tp_flip, grp=grp_of(at["grp"])
        )
        pairs.append((flat, int(np.ravel_multi_index([to[n] for n in names], sizes))))
    return pairs


def make_local(mesh):
    n_role, n_grp, n_tp = (mesh.shape[n] for n in ("role", "grp", "tp"))
    n_near = 2 if n_grp % 2 == 0 else 1
    n_far = n_grp // n_near
    xor_far = n_far & (n_far - 1) == 0
    names = mesh.axis_names

    def send(x, near=0, role=0, tp=0):
        return lax.ppermute(x, names, swap_table(mesh, lambda g: g ^ near, role, tp))

    def send_far(x, k):
        def grp_of(g):
            far, near = divmod(g, n_near)
            return (far ^ k if xor_far else (far + k) % n_far) * n_near + near

        return lax.ppermute(x, names, swap_table(mesh, grp_of, 0, 0))

    def local(
        q_new, k_new, v_new, k_cache, v_cache, cache_len, cycle_start, residual,
        out_proj, norm_gain, router, route_ids, w_gate, w_up, w_down,
    ):
        role, grp, tp = (lax.axis_index(n) for n in ("role", "grp", "tp"))
        tokens, quarter = residual.shape
        topk = route_ids.shape[1]
        experts = n_grp * w_gate.shape[0]
        cap = max(3, tokens * topk // experts + 2)
        far, near = grp // n_near, grp % n_near
        share = role * n_tp + tp
        parts = n_role * n_tp
        place = share.astype(jnp.int32).reshape(1)
        pieces = attend_project(
            place, q_new, k_new, v_new, k_cache, v_cache, cache_len, cycle_start, out_proj.T, parts
        )
        moved = []
        for k in range(1, parts):
            moved.append(send(pieces[k], role=k // n_tp, tp=k % n_tp))
        gain = lax.dynamic_slice_in_dim(norm_gain, share * quarter, quarter, 0).reshape(1, quarter)
        attended, packed = run_pack(pieces[0], moved, residual, gain, router.T, route_ids.T)
        blocks = [packed] + [send_far(packed, k) for k in range(1, n_far)]
        experts_near = jnp.stack([far * n_near + (near ^ j) for j in range(n_near)])
        rows, picks = run_select(
            experts_near.astype(jnp.int32), blocks, n_near, cap, topk, quarter
        )
        arrived = {(0, 0): rows[0]}
        for j in range(n_near):
            for i in range(n_role):
                if (j, i) != (0, 0):
                    arrived[j, i] = send(rows[j], near=j, role=i)
        half = jnp.stack(
            [jnp.concatenate([arrived[j, i] for j in range(n_near)], 0) for i in range(n_role)]
        )
        other = send(half, tp=1)
        place = jnp.stack([share, grp]).astype(jnp.int32)
        gate_turned, up_turned = jnp.swapaxes(w_gate, 1, 2), jnp.swapaxes(w_up, 1, 2)
        partials = run_first(place, half, gate_turned, up_turned, quarter, n_tp)
        sent, activated, weight = run_second(
            place, half, other, partials, gate_turned, up_turned, w_down, quarter, topk, n_tp
        )
        returned = send(sent, tp=1)
        kept = run_third(place, activated, weight, w_down, n_role, quarter, n_tp)
        acc = kept.astype(jnp.float32) + returned.astype(jnp.float32)
        acc = acc.astype(jnp.bfloat16).reshape(n_role, n_near, n_far * cap, quarter)
        back = []
        for j in range(n_near):
            for i in range(n_role):
                piece = acc[i, j]
                if (j, i) != (0, 0):
                    piece = send(piece, near=j, role=i)
                back.append(piece)
        spread = run_spread(back, picks, n_role, n_far)
        mix = spread[0].astype(jnp.float32)
        for k in range(1, n_far):
            mix = mix + send_far(spread[k], k if xor_far else n_far - k).astype(jnp.float32)
        return (attended, mix.astype(jnp.bfloat16))

    return local


def solution(mesh):
    placed = (
        P("grp", ("role", "tp")),
        P("grp", ("role", "tp")),
        P("grp", ("role", "tp")),
        P("grp", None, ("role", "tp")),
        P("grp", None, ("role", "tp")),
        P("grp"),
        P("grp"),
        P("grp", ("role", "tp")),
        P(("role", "tp"), None),
        P(),
        P(("role", "tp"), None),
        P("grp", None),
        P("grp", None, ("role", "tp")),
        P("grp", None, ("role", "tp")),
        P("grp", ("role", "tp"), None),
    )
    local = make_local(mesh)

    return jax.shard_map(
        local,
        mesh=mesh,
        in_specs=placed,
        out_specs=(P("grp", ("role", "tp")), P("grp", ("role", "tp"))),
        check_vma=False,
    )
```

```python
import functools
import math

import jax
import jax.numpy as jnp
import numpy as np
from jax import lax
from jax.experimental import pallas as pl
from jax.experimental.pallas import tpu as pltpu
from jax.sharding import PartitionSpec as P


HEADS = 64
KV_HEADS = 8
HD = 64


epsilon = 1e-05
COVER = 1 << 33


def attend_kernel(
    len_hbm, start_hbm, q_hbm, kn_hbm, vn_hbm, k_hbm, v_hbm, wo_hbm,
    *rest, grouped, chunks, parts, n_tp,
):
    share = lax.axis_index("role") * n_tp + lax.axis_index("tp")
    early = parts // 2
    outs, (stacked_ref, later_ref), rest = rest[:early], rest[early : early + 2], rest[early + 2 :]
    len_ref, start_ref, q_ref, kn_ref, vn_ref, kbuf, vbuf, wobuf = rest[:8]
    queries, heads, scores, products, small, ksem, vsem, wsem = rest[8:]
    tokens, window, lanes = k_hbm.shape
    pairs = (
        (q_hbm, q_ref), (kn_hbm, kn_ref), (vn_hbm, vn_ref), (len_hbm, len_ref),
        (start_hbm, start_ref),
    )
    firsts = [pltpu.make_async_copy(a, b, small.at[n]) for n, (a, b) in enumerate(pairs)]
    for copy in firsts:
        copy.start()
    n_heads = q_ref.shape[1] // HD
    step = tokens // chunks
    rows = wo_hbm.shape[0] // parts

    def kcopy(n):
        at = pl.ds(n * step, step)
        return pltpu.make_async_copy(k_hbm.at[at], kbuf.at[at], ksem.at[n])

    def vcopy(n):
        at = pl.ds(n * step, step)
        return pltpu.make_async_copy(v_hbm.at[at], vbuf.at[at], vsem.at[n])

    def wrows(k):
        return pl.ds(pl.multiple_of((share ^ k) * rows, 16), rows)

    def wcopy(k):
        target = wobuf.at[k - early] if k >= early else later_ref.at[k]
        return pltpu.make_async_copy(wo_hbm.at[wrows(k)], target, wsem.at[k])

    for n in range(chunks):
        kcopy(n).start()
        vcopy(n).start()
    for k in reversed(range(early, parts)):
        wcopy(k).start()
    for copy in firsts:
        copy.wait()
    lane = lax.broadcasted_iota(jnp.int32, (tokens, lanes), 1)
    per = lanes // HD

    def shifted(x, source, target):
        if source == target:
            return x
        return pltpu.roll(x, ((target - source) * HD) % lanes, 1)

    for h in range(n_heads):
        at = h // per * lanes
        x = q_ref[:, at : at + lanes].astype(jnp.float32)
        kv = h // grouped
        x = jnp.where(lane // HD == kv, shifted(x, h % per, kv), 0.0)
        queries[h * tokens : (h + 1) * tokens, :] = x
    factor = HD ** (-0.5)
    slots = lax.broadcasted_iota(jnp.int32, (1, window), 1)
    own_keys = kn_ref[...].astype(jnp.float32)
    own_values = vn_ref[...].astype(jnp.float32)
    block = step * n_heads
    for n in range(chunks):
        kcopy(n).wait()
        if n == 0:
            for k in reversed(range(early)):
                wcopy(k).start()
        for t in range(n * step, (n + 1) * step):
            query = queries[pl.ds(t, n_heads, stride=tokens), :]
            dots = lax.dot_general(
                query.astype(jnp.bfloat16), kbuf[t], (((1,), (1,)), ((), ())),
                preferred_element_type=jnp.float32,
            )
            age = slots - start_ref[t]
            age = jnp.where(age < 0, age + window, age)
            at = pl.ds(t * n_heads, n_heads)
            scores[at, :] = jnp.where(age < len_ref[t], factor * dots, -1e30)
            products[at, :] = query * own_keys[t : t + 1, :]
    for n in range(chunks):
        at = pl.ds(n * block, block)
        masked = scores[at, :]
        own = factor * jnp.sum(products[at, :], axis=1, keepdims=True)
        highest = jnp.maximum(jnp.max(masked, axis=1, keepdims=True), own)
        lifted = jnp.exp(masked - highest)
        own_lift = jnp.exp(own - highest)
        denominator = jnp.sum(lifted, axis=1, keepdims=True) + own_lift
        weights = (lifted / denominator).astype(jnp.bfloat16)
        own_weight = (own_lift / denominator).astype(jnp.bfloat16).astype(jnp.float32)
        vcopy(n).wait()
        for m in range(step):
            t = n * step + m
            mine = slice(m * n_heads, (m + 1) * n_heads)
            mixed = jnp.dot(weights[mine], vbuf[t], preferred_element_type=jnp.float32)
            mixed = mixed + own_weight[mine] * own_values[t : t + 1, :]
            heads[pl.ds(t, n_heads, stride=tokens), :] = mixed
    columns = []
    for c in range(n_heads // per):
        column = None
        for p in range(per):
            h = c * per + p
            x = shifted(heads[h * tokens : (h + 1) * tokens, :], h // grouped, p)
            column = x if column is None else jnp.where(lane // HD == p, x, column)
        columns.append(column.astype(jnp.bfloat16))
    stacked = jnp.concatenate(columns, axis=1)
    stacked_ref[...] = stacked
    for k in reversed(range(early, parts)):
        wcopy(k).wait()
        piece = lax.dot_general(
            stacked, wobuf[k - early], (((1,), (1,)), ((), ())),
            preferred_element_type=jnp.float32,
        )
        outs[k - early][...] = piece.astype(outs[k - early].dtype)
    for k in reversed(range(early)):
        wcopy(k).wait()


def project_kernel(stacked_ref, later_ref, *outs):
    for k in reversed(range(len(outs))):
        piece = lax.dot_general(
            stacked_ref[...], later_ref[k], (((1,), (1,)), ((), ())),
            preferred_element_type=jnp.float32,
        )
        outs[k][...] = piece.astype(outs[k].dtype)


def attend_project(
    q_new, k_new, v_new, k_cache, v_cache, cache_len, cycle_start, out_proj, parts, n_tp
):
    tokens, window, lanes = k_cache.shape
    n_heads = q_new.shape[1] // HD
    quarter = out_proj.shape[0] // parts
    chunks = 2
    vmem = pl.BlockSpec(memory_space=pltpu.VMEM)
    hbm = pl.BlockSpec(memory_space=pltpu.HBM)
    inputs = [
        pltpu.with_memory_space_constraint(x, pltpu.HBM)
        for x in (
            cache_len, cycle_start, q_new, k_new, v_new, k_cache, v_cache, out_proj
        )
    ]
    early = parts // 2
    piece = jax.ShapeDtypeStruct((tokens, quarter), jnp.bfloat16)
    made = pl.pallas_call(
        functools.partial(
            attend_kernel, grouped=HEADS // KV_HEADS, chunks=chunks, parts=parts, n_tp=n_tp
        ),
        in_specs=[hbm] * 8,
        out_specs=[vmem] * (early + 2),
        out_shape=[piece] * early
        + [
            jax.ShapeDtypeStruct(q_new.shape, jnp.bfloat16),
            jax.ShapeDtypeStruct((parts - early, quarter, q_new.shape[1]), out_proj.dtype),
        ],
        scratch_shapes=[
            pltpu.SMEM(cache_len.shape, jnp.int32),
            pltpu.SMEM(cycle_start.shape, jnp.int32),
            pltpu.VMEM(q_new.shape, q_new.dtype),
            pltpu.VMEM(k_new.shape, k_new.dtype),
            pltpu.VMEM(v_new.shape, v_new.dtype),
            pltpu.VMEM(k_cache.shape, k_cache.dtype),
            pltpu.VMEM(v_cache.shape, v_cache.dtype),
            pltpu.VMEM((parts - early, quarter, q_new.shape[1]), out_proj.dtype),
            pltpu.VMEM((n_heads * tokens, lanes), jnp.float32),
            pltpu.VMEM((n_heads * tokens, lanes), jnp.float32),
            pltpu.VMEM((n_heads * tokens, window), jnp.float32),
            pltpu.VMEM((n_heads * tokens, lanes), jnp.float32),
            pltpu.SemaphoreType.DMA((5,)),
            pltpu.SemaphoreType.DMA((chunks,)),
            pltpu.SemaphoreType.DMA((chunks,)),
            pltpu.SemaphoreType.DMA((parts,)),
        ],
        compiler_params=pltpu.CompilerParams(vmem_limit_bytes=16 << 20),
        name="attend_project",
    )(*inputs)
    first, (stacked, later) = made[:early], made[early:]
    later_call = pl.pallas_call(
        project_kernel,
        in_specs=[vmem, vmem],
        out_specs=[vmem] * early,
        out_shape=[jax.ShapeDtypeStruct((tokens, quarter), jnp.float32)] + [piece] * (early - 1),
        compiler_params=pltpu.CompilerParams(vmem_limit_bytes=8 << 20),
        name="project",
    )
    rest = later_call(stacked, later)
    return list(rest) + list(first)


def for_each_core(n_role, n_tp, body):
    role = lax.axis_index("role")
    slots = [role ^ r for r in range(n_role)]
    for tp in range(n_tp):
        places = [r * n_tp + tp for r in range(n_role)]
        pairs = [r * n_tp + (tp ^ 1) for r in range(n_role)]
        pl.when(lax.axis_index("tp") == tp)(functools.partial(body, slots, places, pairs))


def window_of(place, quarter):
    first, last = place * quarter, (place + 1) * quarter
    start = first // 128 * 128
    return slice(start, last), first - start


def partial_products(refs, places, gate_ref, up_ref, quarter):
    turned = (((1,), (1,)), ((), ()))
    gate_lin = up_lin = 0.0
    for x, p in zip(refs, places):
        at, shift = window_of(p, quarter)
        x = x[:, :quarter]
        if shift:
            x = jnp.concatenate([jnp.zeros((x.shape[0], shift), x.dtype), x], axis=1)
        gate_lin = gate_lin + lax.dot_general(
            x, gate_ref[0, :, at], turned, preferred_element_type=jnp.float32
        )
        up_lin = up_lin + lax.dot_general(
            x, up_ref[0, :, at], turned, preferred_element_type=jnp.float32
        )
    return gate_lin, up_lin


def down_products(activated, place, down_ref, quarter):
    at, shift = window_of(place, quarter)
    result = jnp.dot(activated, down_ref[0, :, at], preferred_element_type=jnp.float32)
    return result[:, shift:].astype(jnp.bfloat16)


def first_kernel(own_ref, gate_ref, up_ref, gate_out, up_out, *, quarter, n_tp):
    n_role = own_ref.shape[0]

    def body(slots, places, pairs):
        gate_out[...], up_out[...] = partial_products(
            [own_ref[i] for i in slots], places, gate_ref, up_ref, quarter
        )

    for_each_core(n_role, n_tp, body)


def second_kernel(
    own_ref, other_ref, gate_in, up_in, gate_ref, up_ref, down_ref, send_ref,
    activated_ref, *, quarter, topk, n_tp,
):
    def body(slots, places, pairs):
        second_body(
            slots, pairs, own_ref, other_ref, gate_in, up_in, gate_ref, up_ref, down_ref,
            send_ref, activated_ref, quarter, topk,
        )

    for_each_core(own_ref.shape[0], n_tp, body)


def second_body(
    slots, pairs, own_ref, other_ref, gate_in, up_in, gate_ref, up_ref, down_ref,
    send_ref, activated_ref, quarter, topk,
):
    n_role, _, _ = own_ref.shape
    tail_at = quarter // 128 * 128
    first = quarter - tail_at
    gate_lin, up_lin = partial_products(
        [other_ref[i] for i in slots], pairs, gate_ref, up_ref, quarter
    )
    tail = 0.0
    for ref in (own_ref, other_ref):
        for i in range(n_role):
            tail = tail + ref[i, :, tail_at:].astype(jnp.float32)
    ids = pltpu.roll(own_ref[0, :, tail_at:].astype(jnp.float32), topk + 1, 1)
    n_stat = 1 + topk
    span = tail.shape[1]
    tail = tail + pltpu.roll(tail, span - n_stat, 1) + pltpu.roll(tail, span - 2 * n_stat, 1)
    at = first + topk
    scale = lax.rsqrt(tail[:, at : at + 1] / down_ref.shape[2] + epsilon)
    lane = lax.broadcasted_iota(jnp.int32, tail.shape, 1)
    chosen = (lane > at) & (lane <= at + topk)
    picked = jnp.where(chosen, tail * scale, -1e30)
    lifted = jnp.exp(picked - jnp.max(picked, axis=1, keepdims=True))
    expert = lax.axis_index("grp").astype(jnp.float32)
    mine = jnp.where(chosen & (ids == expert), lifted, 0.0)
    weight = jnp.sum(mine, axis=1, keepdims=True) / jnp.sum(lifted, axis=1, keepdims=True)
    gate_lin = (gate_lin + gate_in[...]) * scale
    up_lin = (up_lin + up_in[...]) * scale
    activated = gate_lin * jax.nn.sigmoid(1.702 * gate_lin) * (up_lin + 1.0)
    activated = (activated * weight).astype(jnp.bfloat16)
    activated_ref[...] = activated
    for i, p in zip(slots, pairs):
        send_ref[i] = down_products(activated, p, down_ref, quarter)


def third_kernel(activated_ref, down_ref, keep_ref, *, quarter, n_tp):
    n_role = keep_ref.shape[0]

    def body(slots, places, pairs):
        for i, p in zip(slots, places):
            keep_ref[i] = down_products(activated_ref[...], p, down_ref, quarter)

    for_each_core(n_role, n_tp, body)


def run_first(own, w_gate, w_up, quarter, n_tp):
    vmem = pl.BlockSpec(memory_space=pltpu.VMEM)
    partial = jax.ShapeDtypeStruct((own.shape[1], w_gate.shape[1]), jnp.float32)
    return pl.pallas_call(
        functools.partial(first_kernel, quarter=quarter, n_tp=n_tp),
        in_specs=[vmem] * 3,
        out_specs=[vmem, vmem],
        out_shape=[partial, partial],
        compiler_params=pltpu.CompilerParams(vmem_limit_bytes=16 << 20),
        name="expert_first",
    )(own, w_gate, w_up)


def run_second(own, other, partials, w_gate, w_up, w_down, quarter, topk, n_tp):
    n_role, items, _ = own.shape
    vmem = pl.BlockSpec(memory_space=pltpu.VMEM)
    return pl.pallas_call(
        functools.partial(second_kernel, quarter=quarter, topk=topk, n_tp=n_tp),
        in_specs=[vmem] * 7,
        out_specs=[vmem] * 2,
        out_shape=[
            jax.ShapeDtypeStruct((n_role, items, quarter), jnp.bfloat16),
            jax.ShapeDtypeStruct((items, w_gate.shape[1]), jnp.bfloat16),
        ],
        compiler_params=pltpu.CompilerParams(vmem_limit_bytes=24 << 20),
        name="expert_second",
    )(own, other, *partials, w_gate, w_up, w_down)


def run_third(activated, w_down, n_role, quarter, n_tp):
    vmem = pl.BlockSpec(memory_space=pltpu.VMEM)
    items = activated.shape[0]
    return pl.pallas_call(
        functools.partial(third_kernel, quarter=quarter, n_tp=n_tp),
        in_specs=[vmem] * 2,
        out_specs=vmem,
        out_shape=jax.ShapeDtypeStruct((n_role, items, quarter), jnp.bfloat16),
        compiler_params=pltpu.CompilerParams(vmem_limit_bytes=12 << 20),
        name="expert_third",
    )(activated, w_down)


def three_parts(x):
    high = x.astype(jnp.bfloat16).astype(jnp.float32)
    rest = x - high
    middle = rest.astype(jnp.bfloat16).astype(jnp.float32)
    return high, middle, rest - middle


def pack_kernel(own_ref, *rest, moved):
    arrived, rest = rest[:moved], rest[moved:]
    residual_ref, gain_ref, router_ref, ids_ref, stream_ref, packed_ref = rest
    stream = residual_ref[...].astype(jnp.float32) + own_ref[...]
    for ref in arrived:
        stream = stream + ref[...].astype(jnp.float32)
    stream_ref[...] = stream
    tokens, quarter = stream.shape
    topk = ids_ref.shape[0]
    scaled = (stream * gain_ref[...]).astype(jnp.bfloat16)
    squares = jnp.sum(stream * stream, axis=1, keepdims=True)
    logits = lax.dot_general(
        scaled, router_ref[...], (((1,), (1,)), ((), ())), preferred_element_type=jnp.float32
    )
    names = lax.broadcasted_iota(jnp.int32, logits.shape, 1).astype(jnp.float32)
    eye = (
        lax.broadcasted_iota(jnp.int32, (topk, topk), 0)
        == lax.broadcasted_iota(jnp.int32, (topk, topk), 1)
    )
    ids = lax.dot_general(
        ids_ref[...].astype(jnp.float32).astype(jnp.bfloat16), eye.astype(jnp.bfloat16),
        (((0,), (0,)), ((), ())), preferred_element_type=jnp.float32,
    )
    stats = [squares]
    columns = []
    for k in range(topk):
        chosen = ids[:, k : k + 1]
        columns.append(chosen)
        stats.append(jnp.sum(jnp.where(names == chosen, logits, 0.0), axis=1, keepdims=True))
    split = [three_parts(x) for x in stats]
    for p in range(3):
        columns.extend(x[p] for x in split)
    tail_at = quarter // 128 * 128
    first = quarter - tail_at
    packed_ref[:, :quarter] = scaled
    tile = packed_ref[:, tail_at : tail_at + 128]
    lane = lax.broadcasted_iota(jnp.int32, (tokens, 128), 1)
    tail = jnp.zeros((tokens, 128), jnp.float32)
    for c, x in enumerate(columns):
        tail = jnp.where(lane == first + c, x, tail)
    packed_ref[:, tail_at : tail_at + 128] = jnp.where(
        lane < first, tile.astype(jnp.float32), tail
    ).astype(jnp.bfloat16)


def run_pack(own, arrived, residual, gain, router, route_ids):
    tokens, quarter = residual.shape
    vmem = pl.BlockSpec(memory_space=pltpu.VMEM)
    lanes = quarter // 128 * 128 + 128
    assert quarter % 128 + 4 * route_ids.shape[0] + 3 <= 128
    return pl.pallas_call(
        functools.partial(pack_kernel, moved=len(arrived)),
        in_specs=[vmem] * (5 + len(arrived)),
        out_specs=[vmem, vmem],
        out_shape=[
            jax.ShapeDtypeStruct((tokens, quarter), jnp.float32),
            jax.ShapeDtypeStruct((tokens, lanes), jnp.bfloat16),
        ],
        compiler_params=pltpu.CompilerParams(vmem_limit_bytes=4 << 20),
        cost_estimate=pl.CostEstimate(flops=COVER, transcendentals=0, bytes_accessed=1 << 20),
        name="pack",
    )(own, *arrived, residual, gain, router, route_ids)


def select_kernel(*rest, n_far, n_near, cap, topk, quarter):
    blocks, rest = rest[:n_far], rest[n_far:]
    rows, picks = rest[:n_near], rest[n_near:]
    tokens, _ = blocks[0].shape
    tail_at = quarter // 128 * 128
    first = quarter - tail_at
    stacked = jnp.concatenate([ref[...] for ref in blocks], axis=0)
    ids = stacked[:, tail_at:].astype(jnp.float32).T
    n_all = n_far * tokens
    source = lax.broadcasted_iota(jnp.int32, (n_all, n_all), 0)
    target = lax.broadcasted_iota(jnp.int32, (n_all, n_all), 1)
    same = source // tokens == target // tokens
    before = jnp.where(same & (source < target), 1.0, 0.0).astype(jnp.bfloat16)
    slot = lax.broadcasted_iota(jnp.int32, (n_far * cap, n_all), 0).astype(jnp.float32)
    base = lax.broadcasted_iota(jnp.int32, (1, n_all), 1) // tokens * cap
    hits = []
    for j in range(n_near):
        grp = lax.axis_index("grp")
        expert = (grp // n_near * n_near + (grp % n_near ^ j)).astype(jnp.float32)
        hit = jnp.zeros((1, n_all), jnp.float32)
        for k in range(topk):
            hit = hit + jnp.where(ids[first + k : first + k + 1, :] == expert, 1.0, 0.0)
        hits.append(hit)
    line = lax.broadcasted_iota(jnp.int32, (8, n_all), 0)
    table = jnp.zeros((8, n_all), jnp.float32)
    for j in range(n_near):
        table = jnp.where(line == j, hits[j], table)
    ranks = jnp.dot(table.astype(jnp.bfloat16), before, preferred_element_type=jnp.float32)
    chosen = []
    for j in range(n_near):
        at = jnp.where(hits[j] > 0.0, ranks[j : j + 1, :] + base.astype(jnp.float32), -1.0)
        pick = jnp.where(at == slot, 1.0, 0.0).astype(jnp.bfloat16)
        picks[j][...] = pick
        chosen.append(pick)
    result = jnp.dot(
        jnp.concatenate(chosen, axis=0), stacked, preferred_element_type=jnp.float32
    ).astype(jnp.bfloat16)
    for j in range(n_near):
        rows[j][...] = result[j * n_far * cap : (j + 1) * n_far * cap]


def run_select(blocks, n_near, cap, topk, quarter):
    tokens, lanes = blocks[0].shape
    n_far = len(blocks)
    vmem = pl.BlockSpec(memory_space=pltpu.VMEM)
    outs = [jax.ShapeDtypeStruct((n_far * cap, lanes), jnp.bfloat16)] * n_near
    outs += [jax.ShapeDtypeStruct((n_far * cap, n_far * tokens), jnp.bfloat16)] * n_near
    made = pl.pallas_call(
        functools.partial(
            select_kernel, n_far=n_far, n_near=n_near, cap=cap, topk=topk, quarter=quarter
        ),
        in_specs=[vmem] * n_far,
        out_specs=[vmem] * len(outs),
        out_shape=outs,
        compiler_params=pltpu.CompilerParams(vmem_limit_bytes=12 << 20),
        name="select",
    )(*blocks)
    return made[:n_near], made[n_near:]


def spread_kernel(*refs, n_near, n_role, n_far):
    rows, refs = refs[: n_near * n_role], refs[n_near * n_role :]
    picks, outs = refs[:n_near], refs[n_near:]
    total = 0.0
    for j in range(n_near):
        row = 0.0
        for i in range(n_role):
            row = row + rows[j * n_role + i][...].astype(jnp.float32)
        total = total + lax.dot_general(
            picks[j][...], row.astype(jnp.bfloat16), (((0,), (0,)), ((), ())),
            preferred_element_type=jnp.float32,
        )
    tokens = total.shape[0] // n_far
    for n in range(n_far):
        outs[n][...] = total[n * tokens : (n + 1) * tokens].astype(outs[n].dtype)


def run_spread(rows, picks, n_role, n_far):
    n_near = len(picks)
    tokens = picks[0].shape[1] // n_far
    vmem = pl.BlockSpec(memory_space=pltpu.VMEM)
    quarter = rows[0].shape[1]
    kinds = [jnp.float32] + [jnp.bfloat16] * (n_far - 1)
    return pl.pallas_call(
        functools.partial(spread_kernel, n_near=n_near, n_role=n_role, n_far=n_far),
        in_specs=[vmem] * (len(rows) + n_near),
        out_specs=[vmem] * n_far,
        out_shape=[jax.ShapeDtypeStruct((tokens, quarter), kind) for kind in kinds],
        compiler_params=pltpu.CompilerParams(vmem_limit_bytes=12 << 20),
        name="spread",
    )(*rows, *picks)


def swap_table(mesh, grp_of, role_flip, tp_flip):
    names = mesh.axis_names
    sizes = [mesh.shape[n] for n in names]
    pairs = []
    for flat in range(math.prod(sizes)):
        at = dict(zip(names, [int(v) for v in np.unravel_index(flat, sizes)]))
        to = dict(
            role=at["role"] ^ role_flip, tp=at["tp"] ^ tp_flip, grp=grp_of(at["grp"])
        )
        pairs.append((flat, int(np.ravel_multi_index([to[n] for n in names], sizes))))
    return pairs


def make_local(mesh):
    n_role, n_grp, n_tp = (mesh.shape[n] for n in ("role", "grp", "tp"))
    n_near = 2 if n_grp % 2 == 0 else 1
    n_far = n_grp // n_near
    xor_far = n_far & (n_far - 1) == 0
    names = mesh.axis_names

    def send(x, near=0, role=0, tp=0):
        return lax.ppermute(x, names, swap_table(mesh, lambda g: g ^ near, role, tp))

    def send_far(x, k):
        def grp_of(g):
            far, near = divmod(g, n_near)
            return (far ^ k if xor_far else (far + k) % n_far) * n_near + near

        return lax.ppermute(x, names, swap_table(mesh, grp_of, 0, 0))

    def local(
        q_new, k_new, v_new, k_cache, v_cache, cache_len, cycle_start, residual,
        out_proj, norm_gain, router, route_ids, w_gate, w_up, w_down,
    ):
        role, _, tp = (lax.axis_index(n) for n in ("role", "grp", "tp"))
        tokens, quarter = residual.shape
        topk = route_ids.shape[1]
        experts = n_grp * w_gate.shape[0]
        cap = max(3, tokens * topk // experts + 2)
        share = role * n_tp + tp
        parts = n_role * n_tp
        pieces = attend_project(
            q_new, k_new, v_new, k_cache, v_cache, cache_len, cycle_start, out_proj.T, parts, n_tp
        )
        moved = []
        for k in range(1, parts):
            moved.append(send(pieces[k], role=k // n_tp, tp=k % n_tp))
        gain = lax.dynamic_slice_in_dim(norm_gain, share * quarter, quarter, 0).reshape(1, quarter)
        stream, packed = run_pack(pieces[0], moved, residual, gain, router.T, route_ids.T)
        blocks = [packed] + [send_far(packed, k) for k in range(1, n_far)]
        attended = stream.astype(jnp.bfloat16)
        rows, picks = run_select(blocks, n_near, cap, topk, quarter)
        arrived = {(0, 0): rows[0]}
        for j in range(n_near):
            for i in range(n_role):
                if (j, i) != (0, 0):
                    arrived[j, i] = send(rows[j], near=j, role=i)
        half = jnp.stack(
            [jnp.concatenate([arrived[j, i] for j in range(n_near)], 0) for i in range(n_role)]
        )
        other = send(half, tp=1)
        gate_turned, up_turned = jnp.swapaxes(w_gate, 1, 2), jnp.swapaxes(w_up, 1, 2)
        partials = run_first(half, gate_turned, up_turned, quarter, n_tp)
        sent, activated = run_second(
            half, other, partials, gate_turned, up_turned, w_down, quarter, topk, n_tp
        )
        returned = send(sent, tp=1)
        kept = run_third(activated, w_down, n_role, quarter, n_tp)
        acc = kept.astype(jnp.float32) + returned.astype(jnp.float32)
        acc = acc.astype(jnp.bfloat16).reshape(n_role, n_near, n_far * cap, quarter)
        back = []
        for j in range(n_near):
            for i in range(n_role):
                piece = acc[i, j]
                if (j, i) != (0, 0):
                    piece = send(piece, near=j, role=i)
                back.append(piece)
        spread = run_spread(back, picks, n_role, n_far)
        mix = spread[0].astype(jnp.float32)
        for k in range(1, n_far):
            mix = mix + send_far(spread[k], k if xor_far else n_far - k).astype(jnp.float32)
        return (attended, mix.astype(jnp.bfloat16))

    return local


def solution(mesh):
    placed = (
        P("grp", ("role", "tp")),
        P("grp", ("role", "tp")),
        P("grp", ("role", "tp")),
        P("grp", None, ("role", "tp")),
        P("grp", None, ("role", "tp")),
        P("grp"),
        P("grp"),
        P("grp", ("role", "tp")),
        P(("role", "tp"), None),
        P(),
        P(("role", "tp"), None),
        P("grp", None),
        P("grp", None, ("role", "tp")),
        P("grp", None, ("role", "tp")),
        P("grp", ("role", "tp"), None),
    )
    local = make_local(mesh)

    return jax.shard_map(
        local,
        mesh=mesh,
        in_specs=placed,
        out_specs=(P("grp", ("role", "tp")), P("grp", ("role", "tp"))),
        check_vma=False,
    )
```

```python
import functools
import math

import jax
import jax.numpy as jnp
import numpy as np
from jax import lax
from jax.experimental import pallas as pl
from jax.experimental.pallas import tpu as pltpu
from jax.sharding import PartitionSpec as P


HEADS = 64
KV_HEADS = 8
HD = 64


epsilon = 1e-05
COVER = 1 << 33


def attend_kernel(
    len_hbm, start_hbm, q_hbm, kn_hbm, vn_hbm, k_hbm, v_hbm, wo_hbm,
    *rest, grouped, chunks, parts, n_tp,
):
    share = lax.axis_index("role") * n_tp + lax.axis_index("tp")
    early = parts // 2
    outs, (stacked_ref, later_ref), rest = rest[:early], rest[early : early + 2], rest[early + 2 :]
    len_ref, start_ref, q_ref, kn_ref, vn_ref, kbuf, vbuf, wobuf = rest[:8]
    queries, heads, scores, products, small, ksem, vsem, wsem = rest[8:]
    tokens, window, lanes = k_hbm.shape
    pairs = (
        (q_hbm, q_ref), (kn_hbm, kn_ref), (vn_hbm, vn_ref), (len_hbm, len_ref),
        (start_hbm, start_ref),
    )
    firsts = [pltpu.make_async_copy(a, b, small.at[n]) for n, (a, b) in enumerate(pairs)]
    for copy in firsts:
        copy.start()
    n_heads = q_ref.shape[1] // HD
    step = tokens // chunks
    rows = wo_hbm.shape[0] // parts

    def kcopy(n):
        at = pl.ds(n * step, step)
        return pltpu.make_async_copy(k_hbm.at[at], kbuf.at[at], ksem.at[n])

    def vcopy(n):
        at = pl.ds(n * step, step)
        return pltpu.make_async_copy(v_hbm.at[at], vbuf.at[at], vsem.at[n])

    def wrows(k):
        return pl.ds(pl.multiple_of((share ^ k) * rows, 16), rows)

    def wcopy(k):
        target = wobuf.at[k - early] if k >= early else later_ref.at[k]
        return pltpu.make_async_copy(wo_hbm.at[wrows(k)], target, wsem.at[k])

    for n in range(chunks):
        kcopy(n).start()
        vcopy(n).start()
    for k in reversed(range(early, parts)):
        wcopy(k).start()
    for copy in firsts:
        copy.wait()
    lane = lax.broadcasted_iota(jnp.int32, (tokens, lanes), 1)
    per = lanes // HD

    def shifted(x, source, target):
        if source == target:
            return x
        return pltpu.roll(x, ((target - source) * HD) % lanes, 1)

    for h in range(n_heads):
        at = h // per * lanes
        x = q_ref[:, at : at + lanes].astype(jnp.float32)
        kv = h // grouped
        x = jnp.where(lane // HD == kv, shifted(x, h % per, kv), 0.0)
        queries[h * tokens : (h + 1) * tokens, :] = x
    factor = HD ** (-0.5)
    slots = lax.broadcasted_iota(jnp.int32, (1, window), 1)
    own_keys = kn_ref[...].astype(jnp.float32)
    own_values = vn_ref[...].astype(jnp.float32)
    block = step * n_heads
    for n in range(chunks):
        kcopy(n).wait()
        if n == 0:
            for k in reversed(range(early)):
                wcopy(k).start()
        for t in range(n * step, (n + 1) * step):
            query = queries[pl.ds(t, n_heads, stride=tokens), :]
            dots = lax.dot_general(
                query.astype(jnp.bfloat16), kbuf[t], (((1,), (1,)), ((), ())),
                preferred_element_type=jnp.float32,
            )
            age = slots - start_ref[t]
            age = jnp.where(age < 0, age + window, age)
            at = pl.ds(t * n_heads, n_heads)
            scores[at, :] = jnp.where(age < len_ref[t], factor * dots, -1e30)
            products[at, :] = query * own_keys[t : t + 1, :]
    for n in range(chunks):
        at = pl.ds(n * block, block)
        masked = scores[at, :]
        own = factor * jnp.sum(products[at, :], axis=1, keepdims=True)
        highest = jnp.maximum(jnp.max(masked, axis=1, keepdims=True), own)
        lifted = jnp.exp(masked - highest)
        own_lift = jnp.exp(own - highest)
        denominator = jnp.sum(lifted, axis=1, keepdims=True) + own_lift
        weights = (lifted / denominator).astype(jnp.bfloat16)
        own_weight = (own_lift / denominator).astype(jnp.bfloat16).astype(jnp.float32)
        vcopy(n).wait()
        for m in range(step):
            t = n * step + m
            mine = slice(m * n_heads, (m + 1) * n_heads)
            mixed = jnp.dot(weights[mine], vbuf[t], preferred_element_type=jnp.float32)
            mixed = mixed + own_weight[mine] * own_values[t : t + 1, :]
            heads[pl.ds(t, n_heads, stride=tokens), :] = mixed
    columns = []
    for c in range(n_heads // per):
        column = None
        for p in range(per):
            h = c * per + p
            x = shifted(heads[h * tokens : (h + 1) * tokens, :], h // grouped, p)
            column = x if column is None else jnp.where(lane // HD == p, x, column)
        columns.append(column.astype(jnp.bfloat16))
    stacked = jnp.concatenate(columns, axis=1)
    stacked_ref[...] = stacked
    for k in reversed(range(early, parts)):
        wcopy(k).wait()
        piece = lax.dot_general(
            stacked, wobuf[k - early], (((1,), (1,)), ((), ())),
            preferred_element_type=jnp.float32,
        )
        outs[k - early][...] = piece.astype(outs[k - early].dtype)
    for k in reversed(range(early)):
        wcopy(k).wait()


def project_kernel(stacked_ref, later_ref, *outs):
    for k in reversed(range(len(outs))):
        piece = lax.dot_general(
            stacked_ref[...], later_ref[k], (((1,), (1,)), ((), ())),
            preferred_element_type=jnp.float32,
        )
        outs[k][...] = piece.astype(outs[k].dtype)


def attend_project(
    q_new, k_new, v_new, k_cache, v_cache, cache_len, cycle_start, out_proj, parts, n_tp
):
    tokens, window, lanes = k_cache.shape
    n_heads = q_new.shape[1] // HD
    quarter = out_proj.shape[0] // parts
    chunks = 2
    vmem = pl.BlockSpec(memory_space=pltpu.VMEM)
    hbm = pl.BlockSpec(memory_space=pltpu.HBM)
    inputs = [
        pltpu.with_memory_space_constraint(x, pltpu.HBM)
        for x in (
            cache_len, cycle_start, q_new, k_new, v_new, k_cache, v_cache, out_proj
        )
    ]
    early = parts // 2
    piece = jax.ShapeDtypeStruct((tokens, quarter), jnp.bfloat16)
    made = pl.pallas_call(
        functools.partial(
            attend_kernel, grouped=HEADS // KV_HEADS, chunks=chunks, parts=parts, n_tp=n_tp
        ),
        in_specs=[hbm] * 8,
        out_specs=[vmem] * (early + 2),
        out_shape=[piece] * early
        + [
            jax.ShapeDtypeStruct(q_new.shape, jnp.bfloat16),
            jax.ShapeDtypeStruct((parts - early, quarter, q_new.shape[1]), out_proj.dtype),
        ],
        scratch_shapes=[
            pltpu.SMEM(cache_len.shape, jnp.int32),
            pltpu.SMEM(cycle_start.shape, jnp.int32),
            pltpu.VMEM(q_new.shape, q_new.dtype),
            pltpu.VMEM(k_new.shape, k_new.dtype),
            pltpu.VMEM(v_new.shape, v_new.dtype),
            pltpu.VMEM(k_cache.shape, k_cache.dtype),
            pltpu.VMEM(v_cache.shape, v_cache.dtype),
            pltpu.VMEM((parts - early, quarter, q_new.shape[1]), out_proj.dtype),
            pltpu.VMEM((n_heads * tokens, lanes), jnp.float32),
            pltpu.VMEM((n_heads * tokens, lanes), jnp.float32),
            pltpu.VMEM((n_heads * tokens, window), jnp.float32),
            pltpu.VMEM((n_heads * tokens, lanes), jnp.float32),
            pltpu.SemaphoreType.DMA((5,)),
            pltpu.SemaphoreType.DMA((chunks,)),
            pltpu.SemaphoreType.DMA((chunks,)),
            pltpu.SemaphoreType.DMA((parts,)),
        ],
        compiler_params=pltpu.CompilerParams(vmem_limit_bytes=16 << 20),
        name="attend_project",
    )(*inputs)
    first, (stacked, later) = made[:early], made[early:]
    later_call = pl.pallas_call(
        project_kernel,
        in_specs=[vmem, vmem],
        out_specs=[vmem] * early,
        out_shape=[jax.ShapeDtypeStruct((tokens, quarter), jnp.float32)] + [piece] * (early - 1),
        compiler_params=pltpu.CompilerParams(vmem_limit_bytes=8 << 20),
        name="project",
    )
    rest = later_call(stacked, later)
    return list(rest) + list(first)


def for_each_core(n_role, n_tp, body):
    role = lax.axis_index("role")
    slots = [role ^ r for r in range(n_role)]
    for tp in range(n_tp):
        places = [r * n_tp + tp for r in range(n_role)]
        pairs = [r * n_tp + (tp ^ 1) for r in range(n_role)]
        pl.when(lax.axis_index("tp") == tp)(functools.partial(body, slots, places, pairs))


def window_of(place, quarter):
    first, last = place * quarter, (place + 1) * quarter
    start = first // 128 * 128
    return slice(start, last), first - start


def partial_products(refs, places, gate_ref, up_ref, quarter):
    turned = (((1,), (1,)), ((), ()))
    gate_lin = up_lin = 0.0
    for x, p in zip(refs, places):
        at, shift = window_of(p, quarter)
        x = x[:, :quarter]
        if shift:
            x = jnp.concatenate([jnp.zeros((x.shape[0], shift), x.dtype), x], axis=1)
        gate_lin = gate_lin + lax.dot_general(
            x, gate_ref[0, :, at], turned, preferred_element_type=jnp.float32
        )
        up_lin = up_lin + lax.dot_general(
            x, up_ref[0, :, at], turned, preferred_element_type=jnp.float32
        )
    return gate_lin, up_lin


def down_products(activated, place, down_ref, quarter):
    at, shift = window_of(place, quarter)
    result = jnp.dot(activated, down_ref[0, :, at], preferred_element_type=jnp.float32)
    return result[:, shift:].astype(jnp.bfloat16)


def first_kernel(own_ref, gate_ref, up_ref, gate_out, up_out, *, quarter, n_tp):
    n_role = own_ref.shape[0]

    def body(slots, places, pairs):
        gate_out[...], up_out[...] = partial_products(
            [own_ref[i] for i in slots], places, gate_ref, up_ref, quarter
        )

    for_each_core(n_role, n_tp, body)


def second_kernel(
    own_ref, other_ref, gate_in, up_in, gate_ref, up_ref, down_ref, send_ref,
    activated_ref, *, quarter, topk, n_tp,
):
    def body(slots, places, pairs):
        second_body(
            slots, pairs, own_ref, other_ref, gate_in, up_in, gate_ref, up_ref, down_ref,
            send_ref, activated_ref, quarter, topk,
        )

    for_each_core(own_ref.shape[0], n_tp, body)


def second_body(
    slots, pairs, own_ref, other_ref, gate_in, up_in, gate_ref, up_ref, down_ref,
    send_ref, activated_ref, quarter, topk,
):
    n_role, _, _ = own_ref.shape
    tail_at = quarter // 128 * 128
    first = quarter - tail_at
    gate_lin, up_lin = partial_products(
        [other_ref[i] for i in slots], pairs, gate_ref, up_ref, quarter
    )
    tail = 0.0
    for ref in (own_ref, other_ref):
        for i in range(n_role):
            tail = tail + ref[i, :, tail_at:].astype(jnp.float32)
    ids = pltpu.roll(own_ref[0, :, tail_at:].astype(jnp.float32), topk + 1, 1)
    n_stat = 1 + topk
    span = tail.shape[1]
    tail = tail + pltpu.roll(tail, span - n_stat, 1) + pltpu.roll(tail, span - 2 * n_stat, 1)
    at = first + topk
    scale = lax.rsqrt(tail[:, at : at + 1] / down_ref.shape[2] + epsilon)
    lane = lax.broadcasted_iota(jnp.int32, tail.shape, 1)
    chosen = (lane > at) & (lane <= at + topk)
    picked = jnp.where(chosen, tail * scale, -1e30)
    lifted = jnp.exp(picked - jnp.max(picked, axis=1, keepdims=True))
    expert = lax.axis_index("grp").astype(jnp.float32)
    mine = jnp.where(chosen & (ids == expert), lifted, 0.0)
    weight = jnp.sum(mine, axis=1, keepdims=True) / jnp.sum(lifted, axis=1, keepdims=True)
    gate_lin = (gate_lin + gate_in[...]) * scale
    up_lin = (up_lin + up_in[...]) * scale
    activated = gate_lin * jax.nn.sigmoid(1.702 * gate_lin) * (up_lin + 1.0)
    activated = (activated * weight).astype(jnp.bfloat16)
    activated_ref[...] = activated
    for i, p in zip(slots, pairs):
        send_ref[i] = down_products(activated, p, down_ref, quarter)


def third_kernel(activated_ref, down_ref, keep_ref, *, quarter, n_tp):
    n_role = keep_ref.shape[0]

    def body(slots, places, pairs):
        for i, p in zip(slots, places):
            keep_ref[i] = down_products(activated_ref[...], p, down_ref, quarter)

    for_each_core(n_role, n_tp, body)


def run_first(own, w_gate, w_up, quarter, n_tp):
    vmem = pl.BlockSpec(memory_space=pltpu.VMEM)
    partial = jax.ShapeDtypeStruct((own.shape[1], w_gate.shape[1]), jnp.float32)
    return pl.pallas_call(
        functools.partial(first_kernel, quarter=quarter, n_tp=n_tp),
        in_specs=[vmem] * 3,
        out_specs=[vmem, vmem],
        out_shape=[partial, partial],
        compiler_params=pltpu.CompilerParams(vmem_limit_bytes=16 << 20),
        name="expert_first",
    )(own, w_gate, w_up)


def run_second(own, other, partials, w_gate, w_up, w_down, quarter, topk, n_tp):
    n_role, items, _ = own.shape
    vmem = pl.BlockSpec(memory_space=pltpu.VMEM)
    return pl.pallas_call(
        functools.partial(second_kernel, quarter=quarter, topk=topk, n_tp=n_tp),
        in_specs=[vmem] * 7,
        out_specs=[vmem] * 2,
        out_shape=[
            jax.ShapeDtypeStruct((n_role, items, quarter), jnp.bfloat16),
            jax.ShapeDtypeStruct((items, w_gate.shape[1]), jnp.bfloat16),
        ],
        compiler_params=pltpu.CompilerParams(vmem_limit_bytes=24 << 20),
        name="expert_second",
    )(own, other, *partials, w_gate, w_up, w_down)


def run_third(activated, w_down, n_role, quarter, n_tp):
    vmem = pl.BlockSpec(memory_space=pltpu.VMEM)
    items = activated.shape[0]
    return pl.pallas_call(
        functools.partial(third_kernel, quarter=quarter, n_tp=n_tp),
        in_specs=[vmem] * 2,
        out_specs=vmem,
        out_shape=jax.ShapeDtypeStruct((n_role, items, quarter), jnp.bfloat16),
        compiler_params=pltpu.CompilerParams(vmem_limit_bytes=12 << 20),
        name="expert_third",
    )(activated, w_down)


def join_kernel(kept_ref, returned_ref, *outs, n_near):
    _, items, _ = kept_ref.shape
    step = items // n_near
    for n, out in enumerate(outs):
        at = pl.ds(n % n_near * step, step)
        total = kept_ref[n // n_near, at].astype(jnp.float32)
        total = total + returned_ref[n // n_near, at].astype(jnp.float32)
        out[...] = total.astype(out.dtype)


def run_join(kept, returned, n_near):
    n_role, items, quarter = kept.shape
    vmem = pl.BlockSpec(memory_space=pltpu.VMEM)
    n_outs = n_role * n_near
    return pl.pallas_call(
        functools.partial(join_kernel, n_near=n_near),
        in_specs=[vmem, vmem],
        out_specs=[vmem] * n_outs,
        out_shape=[jax.ShapeDtypeStruct((items // n_near, quarter), kept.dtype)] * n_outs,
        compiler_params=pltpu.CompilerParams(vmem_limit_bytes=8 << 20),
        name="join",
    )(kept, returned)


def three_parts(x):
    high = x.astype(jnp.bfloat16).astype(jnp.float32)
    rest = x - high
    middle = rest.astype(jnp.bfloat16).astype(jnp.float32)
    return high, middle, rest - middle


def pack_kernel(own_ref, *rest, moved):
    arrived, rest = rest[:moved], rest[moved:]
    residual_ref, gain_ref, router_ref, ids_ref, stream_ref, packed_ref = rest
    stream = residual_ref[...].astype(jnp.float32) + own_ref[...]
    for ref in arrived:
        stream = stream + ref[...].astype(jnp.float32)
    stream_ref[...] = stream
    tokens, quarter = stream.shape
    topk = ids_ref.shape[0]
    scaled = (stream * gain_ref[...]).astype(jnp.bfloat16)
    squares = jnp.sum(stream * stream, axis=1, keepdims=True)
    logits = lax.dot_general(
        scaled, router_ref[...], (((1,), (1,)), ((), ())), preferred_element_type=jnp.float32
    )
    names = lax.broadcasted_iota(jnp.int32, logits.shape, 1).astype(jnp.float32)
    eye = (
        lax.broadcasted_iota(jnp.int32, (topk, topk), 0)
        == lax.broadcasted_iota(jnp.int32, (topk, topk), 1)
    )
    ids = lax.dot_general(
        ids_ref[...].astype(jnp.float32).astype(jnp.bfloat16), eye.astype(jnp.bfloat16),
        (((0,), (0,)), ((), ())), preferred_element_type=jnp.float32,
    )
    stats = [squares]
    columns = []
    for k in range(topk):
        chosen = ids[:, k : k + 1]
        columns.append(chosen)
        stats.append(jnp.sum(jnp.where(names == chosen, logits, 0.0), axis=1, keepdims=True))
    split = [three_parts(x) for x in stats]
    for p in range(3):
        columns.extend(x[p] for x in split)
    tail_at = quarter // 128 * 128
    first = quarter - tail_at
    packed_ref[:, :quarter] = scaled
    tile = packed_ref[:, tail_at : tail_at + 128]
    lane = lax.broadcasted_iota(jnp.int32, (tokens, 128), 1)
    tail = jnp.zeros((tokens, 128), jnp.float32)
    for c, x in enumerate(columns):
        tail = jnp.where(lane == first + c, x, tail)
    packed_ref[:, tail_at : tail_at + 128] = jnp.where(
        lane < first, tile.astype(jnp.float32), tail
    ).astype(jnp.bfloat16)


def run_pack(own, arrived, residual, gain, router, route_ids):
    tokens, quarter = residual.shape
    vmem = pl.BlockSpec(memory_space=pltpu.VMEM)
    lanes = quarter // 128 * 128 + 128
    assert quarter % 128 + 4 * route_ids.shape[0] + 3 <= 128
    return pl.pallas_call(
        functools.partial(pack_kernel, moved=len(arrived)),
        in_specs=[vmem] * (5 + len(arrived)),
        out_specs=[vmem, vmem],
        out_shape=[
            jax.ShapeDtypeStruct((tokens, quarter), jnp.float32),
            jax.ShapeDtypeStruct((tokens, lanes), jnp.bfloat16),
        ],
        compiler_params=pltpu.CompilerParams(vmem_limit_bytes=4 << 20),
        cost_estimate=pl.CostEstimate(flops=COVER, transcendentals=0, bytes_accessed=1 << 20),
        name="pack",
    )(own, *arrived, residual, gain, router, route_ids)


def select_kernel(*rest, n_far, n_near, cap, topk, quarter):
    blocks, rest = rest[:n_far], rest[n_far:]
    rows, picks = rest[:n_near], rest[n_near:]
    tokens, _ = blocks[0].shape
    tail_at = quarter // 128 * 128
    first = quarter - tail_at
    stacked = jnp.concatenate([ref[...] for ref in blocks], axis=0)
    ids = stacked[:, tail_at:].astype(jnp.float32).T
    n_all = n_far * tokens
    source = lax.broadcasted_iota(jnp.int32, (n_all, n_all), 0)
    target = lax.broadcasted_iota(jnp.int32, (n_all, n_all), 1)
    same = source // tokens == target // tokens
    before = jnp.where(same & (source < target), 1.0, 0.0).astype(jnp.bfloat16)
    slot = lax.broadcasted_iota(jnp.int32, (n_far * cap, n_all), 0).astype(jnp.float32)
    base = lax.broadcasted_iota(jnp.int32, (1, n_all), 1) // tokens * cap
    hits = []
    for j in range(n_near):
        grp = lax.axis_index("grp")
        expert = (grp // n_near * n_near + (grp % n_near ^ j)).astype(jnp.float32)
        hit = jnp.zeros((1, n_all), jnp.float32)
        for k in range(topk):
            hit = hit + jnp.where(ids[first + k : first + k + 1, :] == expert, 1.0, 0.0)
        hits.append(hit)
    line = lax.broadcasted_iota(jnp.int32, (8, n_all), 0)
    table = jnp.zeros((8, n_all), jnp.float32)
    for j in range(n_near):
        table = jnp.where(line == j, hits[j], table)
    ranks = jnp.dot(table.astype(jnp.bfloat16), before, preferred_element_type=jnp.float32)
    chosen = []
    for j in range(n_near):
        at = jnp.where(hits[j] > 0.0, ranks[j : j + 1, :] + base.astype(jnp.float32), -1.0)
        pick = jnp.where(at == slot, 1.0, 0.0).astype(jnp.bfloat16)
        picks[j][...] = pick
        chosen.append(pick)
    result = jnp.dot(
        jnp.concatenate(chosen, axis=0), stacked, preferred_element_type=jnp.float32
    ).astype(jnp.bfloat16)
    for j in range(n_near):
        rows[j][...] = result[j * n_far * cap : (j + 1) * n_far * cap]


def run_select(blocks, n_near, cap, topk, quarter):
    tokens, lanes = blocks[0].shape
    n_far = len(blocks)
    vmem = pl.BlockSpec(memory_space=pltpu.VMEM)
    outs = [jax.ShapeDtypeStruct((n_far * cap, lanes), jnp.bfloat16)] * n_near
    outs += [jax.ShapeDtypeStruct((n_far * cap, n_far * tokens), jnp.bfloat16)] * n_near
    made = pl.pallas_call(
        functools.partial(
            select_kernel, n_far=n_far, n_near=n_near, cap=cap, topk=topk, quarter=quarter
        ),
        in_specs=[vmem] * n_far,
        out_specs=[vmem] * len(outs),
        out_shape=outs,
        compiler_params=pltpu.CompilerParams(vmem_limit_bytes=12 << 20),
        name="select",
    )(*blocks)
    return made[:n_near], made[n_near:]


def spread_kernel(*refs, n_near, n_role, n_far):
    rows, refs = refs[: n_near * n_role], refs[n_near * n_role :]
    picks, outs = refs[:n_near], refs[n_near:]
    total = 0.0
    for j in range(n_near):
        row = 0.0
        for i in range(n_role):
            row = row + rows[j * n_role + i][...].astype(jnp.float32)
        total = total + lax.dot_general(
            picks[j][...], row.astype(jnp.bfloat16), (((0,), (0,)), ((), ())),
            preferred_element_type=jnp.float32,
        )
    tokens = total.shape[0] // n_far
    for n in range(n_far):
        outs[n][...] = total[n * tokens : (n + 1) * tokens].astype(outs[n].dtype)


def run_spread(rows, picks, n_role, n_far):
    n_near = len(picks)
    tokens = picks[0].shape[1] // n_far
    vmem = pl.BlockSpec(memory_space=pltpu.VMEM)
    quarter = rows[0].shape[1]
    kinds = [jnp.float32] + [jnp.bfloat16] * (n_far - 1)
    return pl.pallas_call(
        functools.partial(spread_kernel, n_near=n_near, n_role=n_role, n_far=n_far),
        in_specs=[vmem] * (len(rows) + n_near),
        out_specs=[vmem] * n_far,
        out_shape=[jax.ShapeDtypeStruct((tokens, quarter), kind) for kind in kinds],
        compiler_params=pltpu.CompilerParams(vmem_limit_bytes=12 << 20),
        name="spread",
    )(*rows, *picks)


def swap_table(mesh, grp_of, role_flip, tp_flip):
    names = mesh.axis_names
    sizes = [mesh.shape[n] for n in names]
    pairs = []
    for flat in range(math.prod(sizes)):
        at = dict(zip(names, [int(v) for v in np.unravel_index(flat, sizes)]))
        to = dict(
            role=at["role"] ^ role_flip, tp=at["tp"] ^ tp_flip, grp=grp_of(at["grp"])
        )
        pairs.append((flat, int(np.ravel_multi_index([to[n] for n in names], sizes))))
    return pairs


def make_local(mesh):
    n_role, n_grp, n_tp = (mesh.shape[n] for n in ("role", "grp", "tp"))
    n_near = 2 if n_grp % 2 == 0 else 1
    n_far = n_grp // n_near
    xor_far = n_far & (n_far - 1) == 0
    names = mesh.axis_names

    def send(x, near=0, role=0, tp=0):
        return lax.ppermute(x, names, swap_table(mesh, lambda g: g ^ near, role, tp))

    def send_far(x, k):
        def grp_of(g):
            far, near = divmod(g, n_near)
            return (far ^ k if xor_far else (far + k) % n_far) * n_near + near

        return lax.ppermute(x, names, swap_table(mesh, grp_of, 0, 0))

    def local(
        q_new, k_new, v_new, k_cache, v_cache, cache_len, cycle_start, residual,
        out_proj, norm_gain, router, route_ids, w_gate, w_up, w_down,
    ):
        role, _, tp = (lax.axis_index(n) for n in ("role", "grp", "tp"))
        tokens, quarter = residual.shape
        topk = route_ids.shape[1]
        experts = n_grp * w_gate.shape[0]
        cap = max(3, tokens * topk // experts + 2)
        share = role * n_tp + tp
        parts = n_role * n_tp
        pieces = attend_project(
            q_new, k_new, v_new, k_cache, v_cache, cache_len, cycle_start, out_proj.T, parts, n_tp
        )
        moved = []
        for k in range(1, parts):
            moved.append(send(pieces[k], role=k // n_tp, tp=k % n_tp))
        gain = lax.dynamic_slice_in_dim(norm_gain, share * quarter, quarter, 0).reshape(1, quarter)
        stream, packed = run_pack(pieces[0], moved, residual, gain, router.T, route_ids.T)
        blocks = [packed] + [send_far(packed, k) for k in range(1, n_far)]
        attended = stream.astype(jnp.bfloat16)
        rows, picks = run_select(blocks, n_near, cap, topk, quarter)
        arrived = {(0, 0): rows[0]}
        for j in range(n_near):
            for i in range(n_role):
                if (j, i) != (0, 0):
                    arrived[j, i] = send(rows[j], near=j, role=i)
        half = jnp.stack(
            [jnp.concatenate([arrived[j, i] for j in range(n_near)], 0) for i in range(n_role)]
        )
        other = send(half, tp=1)
        gate_turned, up_turned = jnp.swapaxes(w_gate, 1, 2), jnp.swapaxes(w_up, 1, 2)
        partials = run_first(half, gate_turned, up_turned, quarter, n_tp)
        sent, activated = run_second(
            half, other, partials, gate_turned, up_turned, w_down, quarter, topk, n_tp
        )
        returned = send(sent, tp=1)
        kept = run_third(activated, w_down, n_role, quarter, n_tp)
        acc = run_join(kept, returned, n_near)
        back = []
        for j in range(n_near):
            for i in range(n_role):
                piece = acc[i * n_near + j]
                if (j, i) != (0, 0):
                    piece = send(piece, near=j, role=i)
                back.append(piece)
        spread = run_spread(back, picks, n_role, n_far)
        mix = spread[0].astype(jnp.float32)
        for k in range(1, n_far):
            mix = mix + send_far(spread[k], k if xor_far else n_far - k).astype(jnp.float32)
        return (attended, mix.astype(jnp.bfloat16))

    return local


def solution(mesh):
    placed = (
        P("grp", ("role", "tp")),
        P("grp", ("role", "tp")),
        P("grp", ("role", "tp")),
        P("grp", None, ("role", "tp")),
        P("grp", None, ("role", "tp")),
        P("grp"),
        P("grp"),
        P("grp", ("role", "tp")),
        P(("role", "tp"), None),
        P(),
        P(("role", "tp"), None),
        P("grp", None),
        P("grp", None, ("role", "tp")),
        P("grp", None, ("role", "tp")),
        P("grp", ("role", "tp"), None),
    )
    local = make_local(mesh)

    return jax.shard_map(
        local,
        mesh=mesh,
        in_specs=placed,
        out_specs=(P("grp", ("role", "tp")), P("grp", ("role", "tp"))),
        check_vma=False,
    )
```
